32 devices in a mesh: tm: 4 (over x, core), row: 8 (over z, y).
Axes of the slice: x: 2, y: 2, z: 4, core: 2. Of those that a mesh axis runs over, the one named last changes fastest.
Arguments:
- event_counts: int32 [4, 4096, 4096], P('tm', 'row'), may hold values from 0 to 8
- latent_mean: float32 [4, 4096, 4096], P('tm', 'row'), may hold values from -3 to 3
- latent_var: float32 [4, 4096, 4096], P('tm', 'row'), may hold values from 0.05 to 0.6
- eigen_basis: bfloat16 [4096, 4096], P('row', 'tm'), may hold values from -0.09375 to 0.09375
- spectrum: float32 [4096], replicated, may hold values from 0.2 to 2
- correlation: float32 [1], replicated, may hold values from 0.3 to 0.9
- whitened: float32 [4, 8, 128, 4, 4096], P(None, 'row', None, None, 'tm'), may hold values from -6 to 6
Outputs:
- gradient: float32 [4, 8, 128, 4, 4096], P(None, 'row', None, None, 'tm')
The draws below stay inside these ranges and needn't reach their ends.
All inputs are finite; a program needn't handle non-finite values.
Results may differ from the reference program's by a relative error of at most 0.0045.
Values may be sent and summed in bfloat16 or wider, within the bound.
A program may use at most 128 MiB of HBM per device.

```python
import math
import jax
import jax.numpy as jnp
from jax import lax

N = 4096
TS = 4
QB = 128
N_TM = 4
N_ROW = 8


def set_ends(values, rng, smallest, top_value):
    index_at = [jax.random.randint(jax.random.fold_in(rng, axis), (), 0, length) for axis, length in enumerate(values.shape)]
    longest = values.shape.index(max(values.shape))
    next_to = index_at[:longest] + [(index_at[longest] + 1) % values.shape[longest]] + index_at[longest + 1:]
    return values.at[tuple(index_at)].set(smallest).at[tuple(next_to)].set(top_value)


def shard_levels(rng, extent, split, least, largest):
    def one(dim, shards_of):
        draws = jax.random.uniform(jax.random.fold_in(jax.random.fold_in(rng, 6), dim), (shards_of,), jnp.float32, least / len(split), largest / len(split))
        return jnp.repeat(jnp.exp(draws), extent[dim] // shards_of).reshape((-1,) + (1,) * (len(extent) - dim - 1))

    level = one(*split[0])
    for cut in split[1:]:
        level = level * one(*cut)
    return level


def bell_draw(stream_key, dims, width, reach, shards=(), kind=jnp.bfloat16):
    factor_of = shard_levels(stream_key, dims, shards, -0.22, 0.18) if shards else 1.0
    array = jax.random.normal(stream_key, dims, jnp.float32) * width * factor_of
    return jnp.minimum(jnp.maximum(array, -reach), reach).astype(kind)


def setup_inputs(seed: int = 0) -> dict:
    key_list = jax.random.split(jax.random.key(seed), 8)
    event_counts = set_ends(jax.random.randint(key_list[0], (TS, N, N), 0, 9), jax.random.fold_in(key_list[0], 1), 0, 8).astype(jnp.int32)
    latent_mean = bell_draw(key_list[1], (TS, N, N), 0.7, 3.0, ((0, 4), (1, 8)), jnp.float32)
    latent_var = jnp.clip(jnp.exp(math.log(0.6) - 2.4849067 * jax.random.uniform(key_list[2], (TS, N, N), jnp.float32) ** shard_levels(key_list[2], (TS, N, N), ((0, 4), (1, 8)), -0.2, 0.2)), 0.05, 0.6)
    eigen_basis = bell_draw(key_list[3], (N, N), N ** -0.5, 0.09375, ((0, 8), (1, 4)))
    spectrum = jnp.clip(jnp.exp(jax.random.uniform(key_list[4], (N,), jnp.float32, math.log(0.2), math.log(2.0))), 0.2, 2.0)
    correlation = jnp.clip(jax.random.uniform(key_list[5], (1,), jnp.float32, 0.3, 0.9), 0.3, 0.9)
    whitened = bell_draw(key_list[6], (N_TM, N_ROW, QB, TS, N), 1.0, 6.0, ((1, 8), (4, 4)), jnp.float32)
    return dict(event_counts=event_counts, latent_mean=latent_mean, latent_var=latent_var, eigen_basis=eigen_basis, spectrum=spectrum, correlation=correlation, whitened=whitened)


HERMITE_NODES = (-2.0201828704560856, -0.9585724646138185, 0.0, 0.9585724646138185, 2.0201828704560856)
HERMITE_WEIGHTS = (0.019953242059045913, 0.3936193231522412, 0.9453087204829419, 0.3936193231522412, 0.019953242059045913)

def moments(event_counts, latent_mean, latent_var):
    spread = jnp.sqrt(2.0 * latent_var)
    normal = 1.0 / math.sqrt(math.pi)
    points = [latent_mean + spread * abscissa for abscissa in HERMITE_NODES]
    rate_points = [jnp.exp(value) for value in points]
    mean_rate = sum((weight * normal * value for weight, value in zip(HERMITE_WEIGHTS, rate_points)))
    covariance = sum((weight * normal * (node_value - latent_mean) * (value - mean_rate) for weight, node_value, value in zip(HERMITE_WEIGHTS, points, rate_points)))
    rate_var = sum((weight * normal * (value - mean_rate) * (value - mean_rate) for weight, value in zip(HERMITE_WEIGHTS, rate_points)))
    slope_gain = covariance / latent_var
    noise_var = rate_var - slope_gain * covariance + mean_rate
    return slope_gain * (event_counts.astype(latent_mean.dtype) - mean_rate) / noise_var

def time_factor(correlation, total):
    later = jnp.arange(total)[:, None]
    earlier = jnp.arange(total)[None, :]
    distance = jnp.maximum(later - earlier, 0).astype(correlation.dtype)
    lower = jnp.where(later >= earlier, jnp.power(correlation, distance), jnp.zeros_like(distance))
    column_scale = jnp.where(earlier == 0, jnp.ones_like(distance), jnp.sqrt(1.0 - correlation * correlation) * jnp.ones_like(distance))
    return lower * column_scale

def reference(event_counts, latent_mean, latent_var, eigen_basis, spectrum, correlation, whitened):
    pseudo = moments(event_counts, latent_mean, latent_var).astype(jnp.bfloat16)
    factor = time_factor(correlation[0], TS)
    flat = pseudo.reshape(TS, N * N).astype(factor.dtype)
    mixed_field = jnp.dot(factor.T, flat, precision=lax.Precision.HIGHEST).reshape(TS, N, N).astype(jnp.bfloat16)

    def transform(field):
        partial_y = jnp.dot(field, eigen_basis, preferred_element_type=jnp.float32).astype(jnp.bfloat16)
        return jnp.dot(partial_y.T, eigen_basis, preferred_element_type=jnp.float32)
    mode_values = lax.map(transform, mixed_field)
    root_scale = jnp.sqrt(spectrum)
    scaled = root_scale[None, :, None] * root_scale[None, None, :] * mode_values
    gradient = jnp.transpose(scaled, (1, 0, 2)) - whitened.reshape(N, TS, N)
    return gradient.reshape(N_TM, N_ROW, QB, TS, N)
```

```python
import math

import jax
import jax.numpy as jnp
from jax import lax
from jax.experimental import pallas as pl
from jax.experimental.pallas import tpu as pltpu
from jax.sharding import PartitionSpec as P

HERMITE_NODES = (
    -2.0201828704560856,
    -0.9585724646138185,
    0.0,
    0.9585724646138185,
    2.0201828704560856,
)
HERMITE_WEIGHTS = (
    0.019953242059045913,
    0.3936193231522412,
    0.9453087204829419,
    0.3936193231522412,
    0.019953242059045913,
)


def moments(event_counts, latent_mean, latent_var):
    spread = jnp.sqrt(2.0 * latent_var)
    normal = 1.0 / math.sqrt(math.pi)
    points = [latent_mean + spread * abscissa for abscissa in HERMITE_NODES]
    rate_points = [jnp.exp(value) for value in points]
    mean_rate = sum(
        (weight * normal * value for weight, value in zip(HERMITE_WEIGHTS, rate_points))
    )
    covariance = sum(
        (
            weight * normal * (node_value - latent_mean) * (value - mean_rate)
            for weight, node_value, value in zip(HERMITE_WEIGHTS, points, rate_points)
        )
    )
    rate_var = sum(
        (
            weight * normal * (value - mean_rate) * (value - mean_rate)
            for weight, value in zip(HERMITE_WEIGHTS, rate_points)
        )
    )
    slope_gain = covariance / latent_var
    noise_var = rate_var - slope_gain * covariance + mean_rate
    return slope_gain * (event_counts.astype(latent_mean.dtype) - mean_rate) / noise_var


def time_factor(correlation, total):
    later = jnp.arange(total)[:, None]
    earlier = jnp.arange(total)[None, :]
    distance = jnp.maximum(later - earlier, 0).astype(correlation.dtype)
    lower = jnp.where(later >= earlier, jnp.power(correlation, distance), jnp.zeros_like(distance))
    column_scale = jnp.where(
        earlier == 0,
        jnp.ones_like(distance),
        jnp.sqrt(1.0 - correlation * correlation) * jnp.ones_like(distance),
    )
    return lower * column_scale


VMEM_BYTES = 60 * 1024 * 1024
ROW_CHUNKS = 2
Q_CHUNKS = 4


def after(block, value):
    return block + (value * 0.0).astype(block.dtype)


def exchange_step(blocks, axis, bit):
    pairs = [(i, i ^ bit) for i in range(lax.axis_size(axis))]
    return blocks + [(off ^ bit, lax.ppermute(b, axis, pairs)) for off, b in blocks]


def exchange_far(own, axis):
    half = lax.axis_size(axis) // 2
    return exchange_step([(0, own)], axis, half) if half else [(0, own)]


def exchange_near(blocks, axis):
    bit = lax.axis_size(axis) // 4
    while bit:
        blocks = exchange_step(blocks, axis, bit)
        bit //= 2
    return blocks


def first_transform(parts, weights, basis, block_modes, q_chunks):
    row_chunks, total = len(parts), len(parts[0])
    rows, width = parts[0][0].shape
    modes = basis.shape[1]
    tile = min(max(256, block_modes), modes)
    blocks = tile // block_modes
    sub = block_modes // q_chunks

    def kernel(weights_ref, *refs):
        part_refs = refs[: row_chunks * total]
        basis_ref = refs[row_chunks * total]
        out_refs = refs[row_chunks * total + 1 :]
        for c in range(row_chunks):
            fields = [
                jnp.dot(part_refs[c * total + t][...], basis_ref[...], preferred_element_type=jnp.float32)
                for t in range(total)
            ]
            for a in range(total):
                mixed = sum(weights_ref[t, a] * fields[t] for t in range(total))
                turned = mixed.T.astype(jnp.bfloat16).reshape(blocks, block_modes, rows)
                for h in range(q_chunks):
                    out_refs[h][:, a, :, pl.ds(c * rows, rows)] = turned[:, h * sub : (h + 1) * sub, :]

    flat = [p for chunk in parts for p in chunk]
    out = jax.ShapeDtypeStruct((modes // block_modes, total, sub, row_chunks * rows), jnp.bfloat16)
    return pl.pallas_call(
        kernel,
        grid=(modes // tile,),
        in_specs=[pl.BlockSpec(memory_space=pltpu.SMEM)]
        + [pl.BlockSpec((rows, width), lambda i: (0, 0), pipeline_mode=pl.Buffered(1)) for _ in flat]
        + [pl.BlockSpec((width, tile), lambda i: (0, i))],
        out_specs=[pl.BlockSpec((blocks, total, sub, row_chunks * rows), lambda i: (i, 0, 0, 0))] * q_chunks,
        out_shape=[out] * q_chunks,
        compiler_params=pltpu.CompilerParams(vmem_limit_bytes=VMEM_BYTES),
        cost_estimate=pl.CostEstimate(
            flops=2 * total * row_chunks * rows * width * modes,
            bytes_accessed=2 * (total * row_chunks * rows * (width + modes) + width * modes),
            transcendentals=0,
        ),
        name="first_transform",
    )(weights, *flat, basis)


def second_transform(groups, units, basis, scale_y, scale_x, whitened, previous, h, q_chunks):
    count = len(groups)
    sources, total, sub, depth = groups[0].shape
    units_total, _, block_modes, _, band = whitened.shape
    tile = min(256, band)
    width = basis.shape[0]

    def kernel(units_ref, *refs):
        group_refs = refs[:count]
        basis_ref, y_ref, x_ref, whitened_ref = refs[count : count + 4]
        out_ref, done_ref = refs[-2:]
        done_ref[...] = jnp.zeros_like(done_ref)
        for s in range(count):
            left = jnp.concatenate(
                [group_refs[s][r].reshape(total * sub, depth) for r in range(sources)], axis=1
            )
            values = jnp.dot(left, basis_ref[...], preferred_element_type=jnp.float32)
            u = units_ref[s]
            scale = y_ref[u] * x_ref[...]
            for a in range(total):
                out_ref[u, 0, :, a, :] = scale * values[a * sub : (a + 1) * sub] - whitened_ref[u, 0, :, a, :]

    field = pl.BlockSpec((units_total, 1, sub, total, tile), lambda i: (0, 0, h, 0, i))
    operands = [units, *groups, basis, scale_y, scale_x, whitened]
    in_specs = (
        [pl.BlockSpec(memory_space=pltpu.SMEM)]
        + [pl.BlockSpec(g.shape, lambda i: (0, 0, 0, 0), pipeline_mode=pl.Buffered(1)) for g in groups]
        + [
            pl.BlockSpec((width, tile), lambda i: (0, i)),
            pl.BlockSpec((units_total, sub, 1), lambda i: (0, h, 0)),
            pl.BlockSpec((1, tile), lambda i: (0, i)),
            field,
        ]
    )
    aliases = {}
    if previous is not None:
        aliases = {len(operands): 0}
        operands.append(previous)
        in_specs.append(pl.BlockSpec(memory_space=pl.ANY))
    return pl.pallas_call(
        kernel,
        grid=(band // tile,),
        in_specs=in_specs,
        out_specs=[field, pl.BlockSpec((8, 128), lambda i: (0, 0))],
        out_shape=[
            jax.ShapeDtypeStruct(whitened.shape, jnp.float32),
            jax.ShapeDtypeStruct((8, 128), jnp.float32),
        ],
        input_output_aliases=aliases,
        compiler_params=pltpu.CompilerParams(vmem_limit_bytes=VMEM_BYTES),
        cost_estimate=pl.CostEstimate(
            flops=2 * count * total * sub * width * band,
            bytes_accessed=2 * width * (band + count * total * sub) + 8 * count * total * sub * band,
            transcendentals=0,
        ),
        name="second_transform",
    )(*operands)


MESH = pl.DeviceIdType.MESH
FUSED_VMEM_BYTES = 67043328
MOMENT_ROWS = 32
TILE_ORDER = (2, 0, 3, 1)


def flip(value, mask, span):
    result, bit = 0, 1
    while bit < span:
        digit = lax.rem(lax.div(value, bit), 2)
        result = result + ((1 - digit) if mask & bit else digit) * bit
        bit *= 2
    return result


def pseudo_block(counts, mean, var):
    spread = jnp.sqrt(2.0 * var)
    normal = 1.0 / math.sqrt(math.pi)
    h0 = HERMITE_WEIGHTS[2] * normal
    h1 = HERMITE_WEIGHTS[3] * normal
    h2 = HERMITE_WEIGHTS[4] * normal
    d1 = spread * HERMITE_NODES[3]
    d2 = spread * HERMITE_NODES[4]
    level = jnp.exp(mean)
    up1, down1 = jnp.exp(d1), jnp.exp(-d1)
    up2, down2 = jnp.exp(d2), jnp.exp(-d2)
    rate = h0 + h1 * (up1 + down1) + h2 * (up2 + down2)
    cov = (h1 * d1) * (up1 - down1) + (h2 * d2) * (up2 - down2)
    e0 = 1.0 - rate
    e1, e2, e3, e4 = up1 - rate, down1 - rate, up2 - rate, down2 - rate
    scatter = h0 * (e0 * e0) + h1 * (e1 * e1 + e2 * e2) + h2 * (e3 * e3 + e4 * e4)
    slope = cov / var
    noise = level * (scatter - slope * cov) + rate
    return slope * (counts.astype(jnp.float32) - level * rate) / noise


def fused_kernel(
    weights,
    counts,
    mean,
    var,
    basis,
    scale_y,
    scale_x,
    whitened,
    out,
    pbuf,
    ebuf,
    hbuf,
    gbuf,
    acc,
    c_in,
    m_in,
    v_in,
    in_sem,
    own_sem,
    acc_sem,
    self_sem,
    out_sem,
    px_s,
    px_r,
    pc_s,
    pc_r,
    pf_s,
    pf_r,
    eu_s,
    eu_r,
    ed_s,
    ed_r,
    ey_s,
    ey_r,
    at_s,
    at_r,
    gx_s,
    gx_r,
    gc_s,
    gc_r,
    gf_s,
    gf_r,
):
    total, rows, cells = pbuf.shape
    lines = hbuf.shape[0]
    band = ebuf.shape[1]
    block = scale_y.shape[1]
    units = gbuf.shape[0]
    chunk = c_in.shape[1]
    chunks = rows // chunk
    half = rows // 2
    i = lax.axis_index("tm")
    r = lax.axis_index("row")
    z = lax.div(r, 2)
    y = lax.rem(r, 2)
    near = flip(i, 1, units)
    far = flip(i, 2, units)
    cross = flip(i, 3, units)
    side = 2 * z + 1 - y

    def remote(src, dst, send, recv, tm, row):
        return pltpu.make_async_remote_copy(
            src_ref=src, dst_ref=dst, send_sem=send, recv_sem=recv, device_id=(tm, row), device_id_type=MESH
        )

    def fetch(c):
        slot = lax.rem(c, 2)
        at = pl.ds(pl.multiple_of(c * chunk, chunk), chunk)
        return [
            pltpu.make_async_copy(src.at[0, at], dst.at[slot], in_sem.at[n, slot])
            for n, (src, dst) in enumerate(((counts, c_in), (mean, m_in), (var, v_in)))
        ]

    for c in range(2):
        for copy in fetch(c):
            copy.start()
    own_basis = pltpu.make_async_copy(basis, ebuf.at[pl.ds(pl.multiple_of(r * rows, rows), rows)], own_sem)
    own_basis.start()
    fill = pltpu.make_async_copy(whitened.at[:, 0], acc, acc_sem)
    fill.start()

    barrier = pltpu.get_barrier_semaphore()
    for row in range(2 * lines - 1):
        peer = lax.rem(r + 1 + row, 2 * lines)
        pl.semaphore_signal(barrier, inc=1, device_id=(i, peer), device_id_type=MESH)
    for tm in (near, far):
        pl.semaphore_signal(barrier, inc=1, device_id=(tm, r), device_id_type=MESH)
    pl.semaphore_wait(barrier, 2 * lines + 1)

    def piece(line, column, h):
        return ebuf.at[pl.ds(pl.multiple_of((2 * line + column) * rows + h * half, half), half)]

    def basis_up(line, n):
        ref = piece(line, y, n % 2)
        return remote(ref, ref, eu_s.at[n], eu_r.at[n], i, r + 2)

    def basis_down(line, n):
        ref = piece(line, y, n % 2)
        return remote(ref, ref, ed_s.at[n], ed_r.at[n], i, r - 2)

    def basis_side(line, column, h):
        ref = piece(line, column, h)
        return remote(ref, ref, ey_s.at[2 * line + h], ey_r.at[2 * line + h], i, side)

    own_basis.wait()
    for h in range(2):

        @pl.when(z < lines - 1)
        def _():
            basis_up(z, h).start()

        @pl.when(z > 0)
        def _():
            basis_down(z, h).start()

        basis_side(z, y, h).start()

    def relay(n):
        b, h = n // 2, n % 2

        @pl.when(z >= b + 1)
        def _():
            line = z - 1 - b
            basis_up(line, n).wait_recv()

            @pl.when(z < lines - 1)
            def _():
                basis_up(line, n + 2).start()

            basis_side(line, y, h).start()

        @pl.when(z <= lines - 2 - b)
        def _():
            line = z + 1 + b
            basis_down(line, n).wait_recv()

            @pl.when(z > 0)
            def _():
                basis_down(line, n + 2).start()

            basis_side(line, y, h).start()

    def rows_of(t, c):
        return pbuf.at[t, pl.ds(pl.multiple_of(c * chunk, chunk), chunk)]

    def slice_far(t, c):
        return remote(rows_of(t, c), rows_of(t, c), px_s.at[c], px_r.at[c], far, r)

    def slice_near(t, c):
        return remote(rows_of(t, c), rows_of(t, c), pc_s.at[c], pc_r.at[c], near, r)

    def slice_on(t, c):
        return remote(rows_of(t, c), rows_of(t, c), pf_s.at[c], pf_r.at[c], near, r)

    lanes = 512 if cells % 512 == 0 else 128
    per_row = cells // lanes

    def moment_step(c, _):
        slot = lax.rem(c, 2)
        for copy in fetch(c):
            copy.wait()

        def part(n, _):
            top = pl.multiple_of(lax.div(n, per_row) * 16, 16)
            left = pl.multiple_of(lax.rem(n, per_row) * lanes, lanes)
            at = (slot, pl.ds(top, 16), pl.ds(left, lanes))
            value = pseudo_block(c_in[at], m_in[at], v_in[at])
            pbuf[i, pl.ds(pl.multiple_of(c * chunk + top, 16), 16), pl.ds(left, lanes)] = value.astype(pbuf.dtype)
            return 0

        lax.fori_loop(0, (chunk // 16) * per_row, part, 0)

        @pl.when(c + 2 < chunks)
        def _():
            for copy in fetch(c + 2):
                copy.start()

        @pl.when(c > 0)
        def _():
            slice_far(i, c - 1).start()
            slice_near(i, c - 1).start()

        return 0

    def pass_on(c, _):
        slice_far(far, c).wait_recv()
        slice_on(far, c).start()
        return 0

    relays = 2 * (lines - 1)
    lax.fori_loop(0, chunks // 2, moment_step, 0)
    if relays:
        relay(0)
    lax.fori_loop(chunks // 2, chunks, moment_step, 0)
    slice_far(i, chunks - 1).start()
    slice_near(i, chunks - 1).start()
    done = 0
    for n in range(1, relays):
        upto = min(chunks, 2 * n + 1)
        relay(n)
        lax.fori_loop(done, upto, pass_on, 0)
        done = upto
    lax.fori_loop(done, chunks, pass_on, 0)
    for line in range(lines):
        for h in range(2):
            basis_side(line, 1 - y, h).wait_recv()

    def arrive(c, _):
        slice_near(near, c).wait_recv()
        slice_on(cross, c).wait_recv()
        return 0

    lax.fori_loop(0, chunks, arrive, 0)

    span = 256

    def transform(k):
        cols = pl.ds(pl.multiple_of(flip(z, k, lines) * (2 * block), 2 * block), 2 * block)

        def part(c, _):
            at = pl.ds(pl.multiple_of(c * span, span), span)
            fields = [
                jnp.dot(pbuf[t, at, :], ebuf[:, cols], preferred_element_type=jnp.float32) for t in range(total)
            ]
            for a in range(total):
                mixed = sum(weights[t, a] * fields[t] for t in range(total))
                turned = mixed.T.astype(hbuf.dtype)
                for column in range(2):
                    hbuf[k, column, a * block : (a + 1) * block, at] = turned[column * block : (column + 1) * block]
            return 0

        lax.fori_loop(0, rows // span, part, 0)

    def source(code):
        k, other = code // 2, code % 2
        return 2 * flip(z, k, lines) + (1 - y if other else y)

    def push(code):
        k, other = code // 2, code % 2
        column = 1 - y if other else y
        return remote(hbuf.at[k, column], gbuf.at[i, r], at_s.at[code], at_r.at[code], i, source(code))

    def landed(code):
        k, other = code // 2, code % 2
        column = 1 - y if other else y
        return remote(hbuf.at[k, column], gbuf.at[i, source(code)], at_s.at[code], at_r.at[code], i, source(code))

    def block_far(u, code):
        ref = gbuf.at[u, source(code)]
        return remote(ref, ref, gx_s.at[code], gx_r.at[code], far, r)

    def block_near(u, code):
        ref = gbuf.at[u, source(code)]
        return remote(ref, ref, gc_s.at[code], gc_r.at[code], near, r)

    def block_on(u, code):
        ref = gbuf.at[u, source(code)]
        return remote(ref, ref, gf_s.at[code], gf_r.at[code], near, r)

    def spread(code):
        if code:
            landed(code).wait_recv()
        block_far(i, code).start()
        block_near(i, code).start()

    wide = 512 if band % 512 == 0 else band

    def accumulate(u, code, first):
        s = source(code)
        depth = pl.ds(pl.multiple_of(s * rows, rows), rows)

        def part(n, _):
            cols = pl.ds(pl.multiple_of(n * wide, wide), wide)
            values = jnp.dot(gbuf[u, s], ebuf[depth, cols], preferred_element_type=jnp.float32)
            scale = scale_y[u] * scale_x[:, cols]
            for a in range(total):
                term = scale * values[a * block : (a + 1) * block]
                if first:
                    acc[u, :, a, cols] = term - acc[u, :, a, cols]
                else:
                    acc[u, :, a, cols] = term + acc[u, :, a, cols]
            return 0

        lax.fori_loop(0, band // wide, part, 0)

    order = list(TILE_ORDER) if lines == 4 else list(range(lines))
    for k in order:
        transform(k)
        for other in (0, 1):
            if k == 0 and other == 0:
                own = pltpu.make_async_copy(hbuf.at[0, y], gbuf.at[i, r], self_sem)
                own.start()
                own.wait()
                spread(0)
            else:
                push(2 * k + other).start()

    codes = [0, 1]
    ks = [k for k in order if k]
    if lines == 4:
        codes += [4, 2, 5, 3, 6, 7]
    else:
        codes += [2 * k + other for k in ks for other in (0, 1)]
    fill.wait()
    count = len(codes)

    def finish(u, n):
        return pltpu.make_async_copy(acc.at[u], out.at[u, 0], out_sem.at[n])

    for m in range(count + 1):
        if 0 < m < count:
            spread(codes[m])
        if m >= 1:
            code = codes[m - 1]
            accumulate(i, code, m == 1)
            block_near(near, code).wait_recv()
            accumulate(near, code, m == 1)
            if m == count:
                finish(i, 0).start()
                finish(near, 1).start()
            block_far(far, code).wait_recv()
            block_on(far, code).start()
            accumulate(far, code, m == 1)
            if m == count:
                finish(far, 2).start()
            block_on(cross, code).wait_recv()
            accumulate(cross, code, m == 1)
    finish(cross, 3).start()
    for n, u in enumerate((i, near, far, cross)):
        finish(u, n).wait()

    for h in range(2):

        @pl.when(z < lines - 1)
        def _():
            basis_up(z, h).wait_send()

        @pl.when(z > 0)
        def _():
            basis_down(z, h).wait_send()

        basis_side(z, y, h).wait_send()
    for n in range(relays):
        b, h = n // 2, n % 2

        @pl.when(z >= b + 1)
        def _():
            line = z - 1 - b

            @pl.when(z < lines - 1)
            def _():
                basis_up(line, n + 2).wait_send()

            basis_side(line, y, h).wait_send()

        @pl.when(z <= lines - 2 - b)
        def _():
            line = z + 1 + b

            @pl.when(z > 0)
            def _():
                basis_down(line, n + 2).wait_send()

            basis_side(line, y, h).wait_send()

    def sent(c, _):
        slice_far(i, c).wait_send()
        slice_near(i, c).wait_send()
        slice_on(far, c).wait_send()
        return 0

    lax.fori_loop(0, chunks, sent, 0)
    for code in range(count):
        if code:
            push(code).wait_send()
        block_far(i, code).wait_send()
        block_near(i, code).wait_send()
        block_on(far, code).wait_send()


def fused(event_counts, latent_mean, latent_var, basis, weights, scale_y, scale_x, whitened):
    rows, cells = event_counts.shape[1:]
    units, _, block, total, band = whitened.shape
    sources = cells // rows
    lines = sources // 2
    chunks = rows // MOMENT_ROWS
    codes = 2 * lines
    dma = pltpu.SemaphoreType.DMA
    any_space = pl.BlockSpec(memory_space=pl.ANY)
    vmem = pl.BlockSpec(memory_space=pltpu.VMEM)
    return pl.pallas_call(
        fused_kernel,
        in_specs=[pl.BlockSpec(memory_space=pltpu.SMEM)] + [any_space] * 4 + [vmem] * 2 + [any_space],
        out_specs=any_space,
        out_shape=jax.ShapeDtypeStruct(whitened.shape, jnp.float32),
        scratch_shapes=[
            pltpu.VMEM((total, rows, cells), jnp.bfloat16),
            pltpu.VMEM((cells, band), jnp.bfloat16),
            pltpu.VMEM((lines, 2, total * block, rows), jnp.bfloat16),
            pltpu.VMEM((units, sources, total * block, rows), jnp.bfloat16),
            pltpu.VMEM((units, block, total, band), jnp.float32),
            pltpu.VMEM((2, MOMENT_ROWS, cells), jnp.int32),
            pltpu.VMEM((2, MOMENT_ROWS, cells), jnp.float32),
            pltpu.VMEM((2, MOMENT_ROWS, cells), jnp.float32),
            dma((3, 2)),
            dma,
            dma,
            dma,
            dma((4,)),
        ]
        + [dma((chunks,))] * 6
        + [dma((2 * lines,))] * 6
        + [dma((codes,))] * 8,
        compiler_params=pltpu.CompilerParams(
            collective_id=0, has_side_effects=True, vmem_limit_bytes=FUSED_VMEM_BYTES
        ),
        cost_estimate=pl.CostEstimate(
            flops=4 * total * rows * cells * band,
            bytes_accessed=12 * rows * cells + 2 * rows * band + 8 * units * block * total * band,
            transcendentals=7 * rows * cells,
        ),
        name="cox_gradient",
    )(weights, event_counts, latent_mean, latent_var, basis, scale_y, scale_x, whitened)


def fits(event_counts, eigen_basis, whitened, time_count, row_devices):
    rows = event_counts.shape[1]
    units, _, block, total, band = whitened.shape
    power = row_devices >= 2 and row_devices & (row_devices - 1) == 0
    return (
        time_count == units == total == 4
        and power
        and rows % 256 == 0
        and block % 128 == 0
        and band % 256 == 0
    )


def local(event_counts, latent_mean, latent_var, eigen_basis, spectrum, correlation, whitened):
    time_count = lax.axis_size("tm")
    row_devices = lax.axis_size("row")
    here = lax.axis_index("tm")
    total = whitened.shape[3]
    block_modes = whitened.shape[2]
    band_width = eigen_basis.shape[1]
    if fits(event_counts, eigen_basis, whitened, time_count, row_devices):
        weights = time_factor(correlation[0], total)
        scale_x = jnp.sqrt(lax.dynamic_slice_in_dim(spectrum, here * band_width, band_width, 0))[None, :]
        scale_y = jnp.sqrt(
            lax.dynamic_slice_in_dim(
                spectrum.reshape(time_count, row_devices, block_modes), lax.axis_index("row"), 1, 1
            ).reshape(time_count, block_modes, 1)
        )
        return fused(event_counts, latent_mean, latent_var, eigen_basis, weights, scale_y, scale_x, whitened)
    basis = lax.all_gather(eigen_basis, "row", axis=0, tiled=True)
    rows = event_counts.shape[1]
    row_chunks = ROW_CHUNKS if rows // ROW_CHUNKS % 128 == 0 else 1
    q_chunks = Q_CHUNKS if block_modes // Q_CHUNKS % 16 == 0 else 1
    step = rows // row_chunks
    parts = []
    for c in range(row_chunks):
        cut = [x[0, c * step : (c + 1) * step] for x in (event_counts, latent_mean, latent_var)]
        blocks = exchange_near(exchange_far(moments(*cut).astype(jnp.bfloat16), "tm"), "tm")
        parts.append([b for _, b in blocks])
    offsets = jnp.array([off for off, _ in blocks], jnp.int32)
    units = jnp.bitwise_xor(here.astype(jnp.int32), offsets)
    weights = jnp.take(time_factor(correlation[0], total), units, axis=0)
    halves = first_transform(parts, weights, basis, block_modes, q_chunks)
    scale_x = jnp.sqrt(lax.dynamic_slice_in_dim(spectrum, here * band_width, band_width, 0))[None, :]
    scale_y = jnp.sqrt(
        lax.dynamic_slice_in_dim(
            spectrum.reshape(time_count, row_devices, block_modes), lax.axis_index("row"), 1, 1
        ).reshape(time_count, block_modes, 1)
    )
    spread = []
    for h, half in enumerate(halves):
        if h >= 2:
            half = after(half, spread[h - 2][-1][1][0, 0, 0, 0])
        landed = lax.all_to_all(half, "row", split_axis=0, concat_axis=0, tiled=True)
        spread.append(exchange_far(landed, "tm"))
    gradient, done = None, None
    for h, blocks in enumerate(spread):
        if h == q_chunks - 1 and done is not None:
            blocks = blocks[:-1] + [(blocks[-1][0], after(blocks[-1][1], done[0, 0]))]
        groups = [b for _, b in exchange_near(blocks, "tm")]
        gradient, done = second_transform(
            groups, units, basis, scale_y, scale_x, whitened, gradient, h, q_chunks
        )
    return gradient


def solution(mesh):
    return jax.shard_map(
        local,
        mesh=mesh,
        in_specs=(
            P("tm", "row", None),
            P("tm", "row", None),
            P("tm", "row", None),
            P("row", "tm"),
            P(),
            P(),
            P(None, "row", None, None, "tm"),
        ),
        out_specs=P(None, "row", None, None, "tm"),
        check_vma=False,
    )
```

```python
import math

import jax
import jax.numpy as jnp
from jax import lax
from jax.experimental import pallas as pl
from jax.experimental.pallas import tpu as pltpu
from jax.sharding import PartitionSpec as P

HERMITE_NODES = (
    -2.0201828704560856,
    -0.9585724646138185,
    0.0,
    0.9585724646138185,
    2.0201828704560856,
)
HERMITE_WEIGHTS = (
    0.019953242059045913,
    0.3936193231522412,
    0.9453087204829419,
    0.3936193231522412,
    0.019953242059045913,
)


def moments(event_counts, latent_mean, latent_var):
    spread = jnp.sqrt(2.0 * latent_var)
    normal = 1.0 / math.sqrt(math.pi)
    points = [latent_mean + spread * abscissa for abscissa in HERMITE_NODES]
    rate_points = [jnp.exp(value) for value in points]
    mean_rate = sum(
        (weight * normal * value for weight, value in zip(HERMITE_WEIGHTS, rate_points))
    )
    covariance = sum(
        (
            weight * normal * (node_value - latent_mean) * (value - mean_rate)
            for weight, node_value, value in zip(HERMITE_WEIGHTS, points, rate_points)
        )
    )
    rate_var = sum(
        (
            weight * normal * (value - mean_rate) * (value - mean_rate)
            for weight, value in zip(HERMITE_WEIGHTS, rate_points)
        )
    )
    slope_gain = covariance / latent_var
    noise_var = rate_var - slope_gain * covariance + mean_rate
    return slope_gain * (event_counts.astype(latent_mean.dtype) - mean_rate) / noise_var


def time_factor(correlation, total):
    later = jnp.arange(total)[:, None]
    earlier = jnp.arange(total)[None, :]
    distance = jnp.maximum(later - earlier, 0).astype(correlation.dtype)
    lower = jnp.where(later >= earlier, jnp.power(correlation, distance), jnp.zeros_like(distance))
    column_scale = jnp.where(
        earlier == 0,
        jnp.ones_like(distance),
        jnp.sqrt(1.0 - correlation * correlation) * jnp.ones_like(distance),
    )
    return lower * column_scale


VMEM_BYTES = 60 * 1024 * 1024
ROW_CHUNKS = 2
Q_CHUNKS = 4


def after(block, value):
    return block + (value * 0.0).astype(block.dtype)


def exchange_step(blocks, axis, bit):
    pairs = [(i, i ^ bit) for i in range(lax.axis_size(axis))]
    return blocks + [(off ^ bit, lax.ppermute(b, axis, pairs)) for off, b in blocks]


def exchange_far(own, axis):
    half = lax.axis_size(axis) // 2
    return exchange_step([(0, own)], axis, half) if half else [(0, own)]


def exchange_near(blocks, axis):
    bit = lax.axis_size(axis) // 4
    while bit:
        blocks = exchange_step(blocks, axis, bit)
        bit //= 2
    return blocks


def first_transform(parts, weights, basis, block_modes, q_chunks):
    row_chunks, total = len(parts), len(parts[0])
    rows, width = parts[0][0].shape
    modes = basis.shape[1]
    tile = min(max(256, block_modes), modes)
    blocks = tile // block_modes
    sub = block_modes // q_chunks

    def kernel(weights_ref, *refs):
        part_refs = refs[: row_chunks * total]
        basis_ref = refs[row_chunks * total]
        out_refs = refs[row_chunks * total + 1 :]
        for c in range(row_chunks):
            fields = [
                jnp.dot(part_refs[c * total + t][...], basis_ref[...], preferred_element_type=jnp.float32)
                for t in range(total)
            ]
            for a in range(total):
                mixed = sum(weights_ref[t, a] * fields[t] for t in range(total))
                turned = mixed.T.astype(jnp.bfloat16).reshape(blocks, block_modes, rows)
                for h in range(q_chunks):
                    out_refs[h][:, a, :, pl.ds(c * rows, rows)] = turned[:, h * sub : (h + 1) * sub, :]

    flat = [p for chunk in parts for p in chunk]
    out = jax.ShapeDtypeStruct((modes // block_modes, total, sub, row_chunks * rows), jnp.bfloat16)
    return pl.pallas_call(
        kernel,
        grid=(modes // tile,),
        in_specs=[pl.BlockSpec(memory_space=pltpu.SMEM)]
        + [pl.BlockSpec((rows, width), lambda i: (0, 0), pipeline_mode=pl.Buffered(1)) for _ in flat]
        + [pl.BlockSpec((width, tile), lambda i: (0, i))],
        out_specs=[pl.BlockSpec((blocks, total, sub, row_chunks * rows), lambda i: (i, 0, 0, 0))] * q_chunks,
        out_shape=[out] * q_chunks,
        compiler_params=pltpu.CompilerParams(vmem_limit_bytes=VMEM_BYTES),
        cost_estimate=pl.CostEstimate(
            flops=2 * total * row_chunks * rows * width * modes,
            bytes_accessed=2 * (total * row_chunks * rows * (width + modes) + width * modes),
            transcendentals=0,
        ),
        name="first_transform",
    )(weights, *flat, basis)


def second_transform(groups, units, basis, scale_y, scale_x, whitened, previous, h, q_chunks):
    count = len(groups)
    sources, total, sub, depth = groups[0].shape
    units_total, _, block_modes, _, band = whitened.shape
    tile = min(256, band)
    width = basis.shape[0]

    def kernel(units_ref, *refs):
        group_refs = refs[:count]
        basis_ref, y_ref, x_ref, whitened_ref = refs[count : count + 4]
        out_ref, done_ref = refs[-2:]
        done_ref[...] = jnp.zeros_like(done_ref)
        for s in range(count):
            left = jnp.concatenate(
                [group_refs[s][r].reshape(total * sub, depth) for r in range(sources)], axis=1
            )
            values = jnp.dot(left, basis_ref[...], preferred_element_type=jnp.float32)
            u = units_ref[s]
            scale = y_ref[u] * x_ref[...]
            for a in range(total):
                out_ref[u, 0, :, a, :] = scale * values[a * sub : (a + 1) * sub] - whitened_ref[u, 0, :, a, :]

    field = pl.BlockSpec((units_total, 1, sub, total, tile), lambda i: (0, 0, h, 0, i))
    operands = [units, *groups, basis, scale_y, scale_x, whitened]
    in_specs = (
        [pl.BlockSpec(memory_space=pltpu.SMEM)]
        + [pl.BlockSpec(g.shape, lambda i: (0, 0, 0, 0), pipeline_mode=pl.Buffered(1)) for g in groups]
        + [
            pl.BlockSpec((width, tile), lambda i: (0, i)),
            pl.BlockSpec((units_total, sub, 1), lambda i: (0, h, 0)),
            pl.BlockSpec((1, tile), lambda i: (0, i)),
            field,
        ]
    )
    aliases = {}
    if previous is not None:
        aliases = {len(operands): 0}
        operands.append(previous)
        in_specs.append(pl.BlockSpec(memory_space=pl.ANY))
    return pl.pallas_call(
        kernel,
        grid=(band // tile,),
        in_specs=in_specs,
        out_specs=[field, pl.BlockSpec((8, 128), lambda i: (0, 0))],
        out_shape=[
            jax.ShapeDtypeStruct(whitened.shape, jnp.float32),
            jax.ShapeDtypeStruct((8, 128), jnp.float32),
        ],
        input_output_aliases=aliases,
        compiler_params=pltpu.CompilerParams(vmem_limit_bytes=VMEM_BYTES),
        cost_estimate=pl.CostEstimate(
            flops=2 * count * total * sub * width * band,
            bytes_accessed=2 * width * (band + count * total * sub) + 8 * count * total * sub * band,
            transcendentals=0,
        ),
        name="second_transform",
    )(*operands)


MESH = pl.DeviceIdType.MESH
FUSED_VMEM_BYTES = 67043328
MOMENT_ROWS = 32


def flip(value, mask, span):
    result, bit = 0, 1
    while bit < span:
        digit = lax.rem(lax.div(value, bit), 2)
        other = lax.rem(lax.div(mask, bit), 2) if not isinstance(mask, int) else mask // bit % 2
        result = result + lax.rem(digit + other, 2) * bit
        bit *= 2
    return result


def pseudo_block(counts, mean, var):
    spread = jnp.sqrt(2.0 * var)
    normal = 1.0 / math.sqrt(math.pi)
    h0 = HERMITE_WEIGHTS[2] * normal
    h1 = HERMITE_WEIGHTS[3] * normal
    h2 = HERMITE_WEIGHTS[4] * normal
    d1 = spread * HERMITE_NODES[3]
    d2 = spread * HERMITE_NODES[4]
    level = jnp.exp(mean)
    up1, down1 = jnp.exp(d1), jnp.exp(-d1)
    up2, down2 = jnp.exp(d2), jnp.exp(-d2)
    rate = h0 + h1 * (up1 + down1) + h2 * (up2 + down2)
    cov = (h1 * d1) * (up1 - down1) + (h2 * d2) * (up2 - down2)
    e0 = 1.0 - rate
    e1, e2, e3, e4 = up1 - rate, down1 - rate, up2 - rate, down2 - rate
    scatter = h0 * (e0 * e0) + h1 * (e1 * e1 + e2 * e2) + h2 * (e3 * e3 + e4 * e4)
    slope = cov / var
    noise = level * (scatter - slope * cov) + rate
    return slope * (counts.astype(jnp.float32) - level * rate) / noise


def fused_kernel(
    correlation,
    counts,
    mean,
    var,
    basis,
    spectrum_y,
    spectrum_x,
    whitened,
    out,
    pbuf,
    ebuf,
    hbuf,
    gbuf,
    acc,
    c_in,
    m_in,
    v_in,
    scale_y,
    in_sem,
    own_sem,
    acc_sem,
    self_sem,
    out_sem,
    px_s,
    px_r,
    pc_s,
    pc_r,
    pf_s,
    pf_r,
    eu_s,
    eu_r,
    ed_s,
    ed_r,
    ey_s,
    ey_r,
    ez_s,
    ez_r,
    at_s,
    at_r,
    gx_s,
    gx_r,
    gc_s,
    gc_r,
    gf_s,
    gf_r,
):
    total, rows, cells = pbuf.shape
    lines = hbuf.shape[0]
    band = ebuf.shape[1]
    block = scale_y.shape[1]
    span = hbuf.shape[-1]
    units = gbuf.shape[0]
    chunk = c_in.shape[1]
    chunks = rows // chunk
    half = rows // 2
    i = lax.axis_index("tm")
    r = lax.axis_index("row")
    z = lax.div(r, 2)
    y = lax.rem(r, 2)
    near = flip(i, 1, units)
    far = flip(i, 2, units)
    cross = flip(i, 3, units)
    side = 2 * z + 1 - y
    twin = flip(z, 1, lines)

    def remote(src, dst, send, recv, tm, row):
        return pltpu.make_async_remote_copy(
            src_ref=src, dst_ref=dst, send_sem=send, recv_sem=recv, device_id=(tm, row), device_id_type=MESH
        )

    def fetch(c):
        slot = lax.rem(c, 2)
        at = pl.ds(pl.multiple_of(c * chunk, chunk), chunk)
        return [
            pltpu.make_async_copy(src.at[0, at], dst.at[slot], in_sem.at[n, slot])
            for n, (src, dst) in enumerate(((counts, c_in), (mean, m_in), (var, v_in)))
        ]

    for c in range(2):
        for copy in fetch(c):
            copy.start()
    own_basis = pltpu.make_async_copy(basis, ebuf.at[pl.ds(pl.multiple_of(r * rows, rows), rows)], own_sem)
    own_basis.start()
    fill = pltpu.make_async_copy(whitened.at[:, 0], acc, acc_sem)
    fill.start()

    barrier = pltpu.get_barrier_semaphore()
    for row in range(2 * lines - 1):
        peer = lax.rem(r + 1 + row, 2 * lines)
        pl.semaphore_signal(barrier, inc=1, device_id=(i, peer), device_id_type=MESH)
    for tm in (near, far):
        pl.semaphore_signal(barrier, inc=1, device_id=(tm, r), device_id_type=MESH)
    pl.semaphore_wait(barrier, 2 * lines + 1)

    def piece(line, column, h):
        return ebuf.at[pl.ds(pl.multiple_of((2 * line + column) * rows + h * half, half), half)]

    def basis_up(line, n):
        ref = piece(line, y, n % 2)
        return remote(ref, ref, eu_s.at[n], eu_r.at[n], i, r + 2)

    def basis_down(line, n):
        ref = piece(line, y, n % 2)
        return remote(ref, ref, ed_s.at[n], ed_r.at[n], i, r - 2)

    def basis_side(line, column, h):
        ref = piece(line, column, h)
        return remote(ref, ref, ey_s.at[2 * line + h], ey_r.at[2 * line + h], i, side)

    def basis_cross(line, column):
        ref = piece(line, column, 1)
        return remote(ref, ref, ez_s, ez_r, i, 2 * twin + y)

    own_basis.wait()
    for h in range(2):

        @pl.when(z < lines - 1)
        def _():
            basis_up(z, h).start()

        @pl.when(z > 0)
        def _():
            basis_down(z, h).start()

        basis_side(z, y, h).start()

    def beside(line, h, begin):
        copy = basis_side(line, y, h)
        if h == 0:
            (copy.start if begin else copy.wait_send)()
        else:

            @pl.when(line != twin)
            def _():
                (copy.start if begin else copy.wait_send)()

    def relay(n):
        b, h = n // 2, n % 2

        @pl.when(z >= b + 1)
        def _():
            line = z - 1 - b
            basis_up(line, n).wait_recv()

            @pl.when(z < lines - 1)
            def _():
                basis_up(line, n + 2).start()

            beside(line, h, True)

        @pl.when(z <= lines - 2 - b)
        def _():
            line = z + 1 + b
            basis_down(line, n).wait_recv()

            @pl.when(z > 0)
            def _():
                basis_down(line, n + 2).start()

            beside(line, h, True)

    def set_scales():
        for u in range(units):
            line = jnp.sqrt(spectrum_y[u, pl.ds(r, 1), :])
            scale_y[u] = jnp.broadcast_to(line, (128, block)).T

    def rows_of(t, c):
        return pbuf.at[t, pl.ds(pl.multiple_of(c * chunk, chunk), chunk)]

    def slice_far(t, c):
        return remote(rows_of(t, c), rows_of(t, c), px_s.at[c], px_r.at[c], far, r)

    def slice_near(t, c):
        return remote(rows_of(t, c), rows_of(t, c), pc_s.at[c], pc_r.at[c], near, r)

    def slice_on(t, c):
        return remote(rows_of(t, c), rows_of(t, c), pf_s.at[c], pf_r.at[c], near, r)

    lanes = 512 if cells % 512 == 0 else 128
    per_row = cells // lanes

    def moment_step(c, _):
        slot = lax.rem(c, 2)
        for copy in fetch(c):
            copy.wait()

        def part(n, _):
            top = pl.multiple_of(lax.div(n, per_row) * 16, 16)
            left = pl.multiple_of(lax.rem(n, per_row) * lanes, lanes)
            at = (slot, pl.ds(top, 16), pl.ds(left, lanes))
            value = pseudo_block(c_in[at], m_in[at], v_in[at])
            pbuf[i, pl.ds(pl.multiple_of(c * chunk + top, 16), 16), pl.ds(left, lanes)] = value.astype(pbuf.dtype)
            return 0

        lax.fori_loop(0, (chunk // 16) * per_row, part, 0)

        @pl.when(c + 2 < chunks)
        def _():
            for copy in fetch(c + 2):
                copy.start()

        @pl.when(c > 0)
        def _():
            slice_far(i, c - 1).start()
            slice_near(i, c - 1).start()

        return 0

    def pass_on(c, _):
        slice_far(far, c).wait_recv()
        slice_on(far, c).start()
        return 0

    relays = 2 * (lines - 1)
    lax.fori_loop(0, chunks // 2, moment_step, 0)
    relay(0)
    lax.fori_loop(chunks // 2, chunks, moment_step, 0)
    slice_far(i, chunks - 1).start()
    slice_near(i, chunks - 1).start()
    set_scales()
    relay(1)
    basis_side(z, 1 - y, 1).wait_recv()
    basis_cross(z, 1 - y).start()
    done = 0
    for n in range(2, relays):
        upto = min(chunks, 2 * n - 1)
        lax.fori_loop(done, upto, pass_on, 0)
        done = upto
        relay(n)
    half_chunks = span // chunk
    late = max(done, chunks - 2)
    lax.fori_loop(done, late, pass_on, 0)
    for line in range(lines):
        basis_side(line, 1 - y, 0).wait_recv()

        @pl.when(jnp.logical_and(line != twin, line != z))
        def _():
            basis_side(line, 1 - y, 1).wait_recv()

    basis_cross(twin, 1 - y).wait_recv()

    def arrive(c, _):
        slice_near(near, c).wait_recv()
        slice_on(cross, c).wait_recv()
        return 0

    def transform(h, k):
        cols = pl.ds(pl.multiple_of(flip(z, k, lines) * (2 * block), 2 * block), 2 * block)
        at = pl.ds(pl.multiple_of(h * span, span), span)
        fields = [jnp.dot(pbuf[t, at, :], ebuf[:, cols], preferred_element_type=jnp.float32) for t in range(total)]
        decay = correlation[0]
        gain = jnp.sqrt(jnp.full((1, 2 * block), 1.0 - decay * decay, jnp.float32))
        mixed = None
        for a in reversed(range(total)):
            mixed = fields[a] if mixed is None else fields[a] + decay * mixed
            turned = (gain * mixed if a else mixed).T.astype(hbuf.dtype)
            for column in range(2):
                hbuf[k, column, h, a * block : (a + 1) * block, :] = turned[column * block : (column + 1) * block]

    def column_of(other):
        return 1 - y if other else y

    def source(code):
        return 2 * flip(z, code // 2, lines) + column_of(code % 2)

    def push(h, k, other):
        code = 2 * k + other
        peer = 2 * flip(z, k, lines) + column_of(other)
        src = hbuf.at[k, column_of(other), h]
        return remote(src, gbuf.at[i, h, r], at_s.at[h, code], at_r.at[h, code], i, peer)

    def landed(h, code):
        src = hbuf.at[code // 2, column_of(code % 2), h]
        return remote(src, gbuf.at[i, h, source(code)], at_s.at[h, code], at_r.at[h, code], i, source(code))

    def block_far(u, h, code):
        ref = gbuf.at[u, h, source(code)]
        return remote(ref, ref, gx_s.at[h, code], gx_r.at[h, code], far, r)

    def block_near(u, h, code):
        ref = gbuf.at[u, h, source(code)]
        return remote(ref, ref, gc_s.at[h, code], gc_r.at[h, code], near, r)

    def block_on(u, h, code):
        ref = gbuf.at[u, h, source(code)]
        return remote(ref, ref, gf_s.at[h, code], gf_r.at[h, code], near, r)

    def spread(h, code):
        if code:
            landed(h, code).wait_recv()
        block_far(i, h, code).start()
        block_near(i, h, code).start()

    def cleanup(later):
        for h in range(2):

            @pl.when(z < lines - 1)
            def _():
                basis_up(z, h).wait_send()

            @pl.when(z > 0)
            def _():
                basis_down(z, h).wait_send()

            basis_side(z, y, h).wait_send()
        for n in range(relays):
            b, h = n // 2, n % 2

            @pl.when(z >= b + 1)
            def _():
                line = z - 1 - b

                @pl.when(z < lines - 1)
                def _():
                    basis_up(line, n + 2).wait_send()

                beside(line, h, False)

            @pl.when(z <= lines - 2 - b)
            def _():
                line = z + 1 + b

                @pl.when(z > 0)
                def _():
                    basis_down(line, n + 2).wait_send()

                beside(line, h, False)

        def sent(c, _):
            slice_far(i, c).wait_send()
            slice_near(i, c).wait_send()
            slice_on(far, c).wait_send()
            return 0

        basis_cross(z, 1 - y).wait_send()

        lax.fori_loop(0, chunks, sent, 0)
        if later:
            for h, code in sequence:
                if code:
                    push(h, code // 2, code % 2).wait_send()
                block_far(i, h, code).wait_send()
                block_near(i, h, code).wait_send()
                block_on(far, h, code).wait_send()

    wide = 512 if band % 512 == 0 else band

    def accumulate(u, pair, first):
        def part(n, _):
            cols = pl.ds(pl.multiple_of(n * wide, wide), wide)
            values = None
            for h, code in pair:
                s = source(code)
                depth = pl.ds(pl.multiple_of(s * rows + h * span, span), span)
                term = jnp.dot(gbuf[u, h, s], ebuf[depth, cols], preferred_element_type=jnp.float32)
                values = term if values is None else values + term
            left = pl.multiple_of(i * band + n * wide, wide)
            scale = scale_y[u, :, 0:1] * jnp.sqrt(spectrum_x[:, pl.ds(left, wide)])
            for a in range(total):
                term = scale * values[a * block : (a + 1) * block]
                if first:
                    acc[u, :, a, cols] = term - acc[u, :, a, cols]
                else:
                    acc[u, :, a, cols] = term + acc[u, :, a, cols]
            return 0

        lax.fori_loop(0, band // wide, part, 0)

    first_order = [2, 0, 1, 3] if lines == 4 else [0] + list(range(1, lines))
    tiles = len(first_order)
    sequence = []
    for h in range(2):
        sequence += [(h, 2 * k + other) for k in sorted(first_order, key=lambda k: (k != 0, first_order.index(k))) for other in (0, 1)]
    if lines == 4:
        sequence = [(0, 0), (0, 1), (0, 4), (1, 0), (1, 1), (0, 5), (0, 2), (0, 3)]
        sequence += [(0, 6), (0, 7), (1, 4), (1, 5), (1, 2), (1, 3), (1, 6), (1, 7)]
    count = len(sequence)

    def pick(n):
        k = first_order[0]
        for m in range(1, tiles):
            k = jnp.where(n == m, first_order[m], k)
        return k

    lax.fori_loop(0, half_chunks, arrive, 0)

    def tile_step(n, _):
        h = lax.div(n, tiles)
        k = pick(lax.rem(n, tiles))

        @pl.when(n == tiles)
        def _():
            lax.fori_loop(half_chunks, chunks, arrive, 0)

        transform(h, k)

        @pl.when(k == 0)
        def _():
            own = pltpu.make_async_copy(hbuf.at[0, y, h], gbuf.at[i, h, r], self_sem)
            own.start()
            own.wait()
            ref = gbuf.at[i, h, r]
            remote(ref, ref, gx_s.at[h, 0], gx_r.at[h, 0], far, r).start()
            remote(ref, ref, gc_s.at[h, 0], gc_r.at[h, 0], near, r).start()

        @pl.when(k != 0)
        def _():
            push(h, k, 0).start()

        push(h, k, 1).start()

        @pl.when(n == tiles - 1)
        def _():
            lax.fori_loop(late, chunks, pass_on, 0)
            spread(*sequence[1])

        @pl.when(n == tiles)
        def _():
            spread(*sequence[2])

        return 0

    lax.fori_loop(0, 2 * tiles, tile_step, 0)
    fill.wait()

    def finish(u, n):
        return pltpu.make_async_copy(acc.at[u], out.at[u, 0], out_sem.at[n])

    pairs = [sequence[2 * p : 2 * p + 2] for p in range(count // 2)]
    state = {"passed": 0, "near": 0, "local": 0, "remote": 0}

    def forward(upto):
        while state["passed"] < upto:
            h, code = sequence[state["passed"]]
            block_far(far, h, code).wait_recv()
            block_on(far, h, code).start()
            state["passed"] += 1

    def local_pair():
        p = state["local"]
        for h, code in pairs[p]:
            block_near(near, h, code).wait_recv()
        for u in (i, near):
            accumulate(u, pairs[p], p == 0)
        state["local"] += 1

    def remote_pair():
        p = state["remote"]
        accumulate(far, pairs[p], p == 0)
        for h, code in pairs[p]:
            block_on(cross, h, code).wait_recv()
        accumulate(cross, pairs[p], p == 0)
        state["remote"] += 1

    for n in range(3, count):
        if sequence[n][1]:
            spread(*sequence[n])
        if n < 6 and lines == 4:
            continue
        forward(max(0, n - 2))
        if 2 * state["local"] + 1 <= n:
            local_pair()
        if 2 * state["remote"] + 1 <= n - 3:
            remote_pair()
    while state["local"] < count // 2:
        local_pair()
    finish(i, 0).start()
    finish(near, 1).start()
    while state["remote"] < count // 2:
        forward(2 * state["remote"] + 2)
        remote_pair()
    finish(far, 2).start()
    finish(cross, 3).start()
    for n, u in enumerate((i, near, far, cross)):
        finish(u, n).wait()
    cleanup(True)


def fused(event_counts, latent_mean, latent_var, basis, spectrum, correlation, whitened):
    rows, cells = event_counts.shape[1:]
    units, _, block, total, band = whitened.shape
    sources = cells // rows
    lines = sources // 2
    chunks = rows // MOMENT_ROWS
    span = rows // 2
    dma = pltpu.SemaphoreType.DMA
    any_space = pl.BlockSpec(memory_space=pl.ANY)
    vmem = pl.BlockSpec(memory_space=pltpu.VMEM)
    return pl.pallas_call(
        fused_kernel,
        in_specs=[pl.BlockSpec(memory_space=pltpu.SMEM)] + [any_space] * 4 + [vmem] * 2 + [any_space],
        out_specs=any_space,
        out_shape=jax.ShapeDtypeStruct(whitened.shape, jnp.float32),
        scratch_shapes=[
            pltpu.VMEM((total, rows, cells), jnp.bfloat16),
            pltpu.VMEM((cells, band), jnp.bfloat16),
            pltpu.VMEM((lines, 2, 2, total * block, span), jnp.bfloat16),
            pltpu.VMEM((units, 2, sources, total * block, span), jnp.bfloat16),
            pltpu.VMEM((units, block, total, band), jnp.float32),
            pltpu.VMEM((2, MOMENT_ROWS, cells), jnp.int32),
            pltpu.VMEM((2, MOMENT_ROWS, cells), jnp.float32),
            pltpu.VMEM((2, MOMENT_ROWS, cells), jnp.float32),
            pltpu.VMEM((units, block, 128), jnp.float32),
            dma((3, 2)),
            dma,
            dma,
            dma,
            dma((4,)),
        ]
        + [dma((chunks,))] * 6
        + [dma((2 * lines,))] * 6
        + [dma] * 2
        + [dma((2, sources))] * 8,
        compiler_params=pltpu.CompilerParams(
            collective_id=0, has_side_effects=True, vmem_limit_bytes=FUSED_VMEM_BYTES
        ),
        cost_estimate=pl.CostEstimate(
            flops=4 * total * rows * cells * band,
            bytes_accessed=12 * rows * cells + 2 * rows * band + 8 * units * block * total * band,
            transcendentals=7 * rows * cells,
        ),
        name="cox_gradient",
    )(
        correlation,
        event_counts,
        latent_mean,
        latent_var,
        basis,
        spectrum.reshape(units, sources, block),
        spectrum[None, :],
        whitened,
    )


def fits(event_counts, eigen_basis, whitened, time_count, row_devices):
    rows = event_counts.shape[1]
    units, _, block, total, band = whitened.shape
    power = row_devices >= 4 and row_devices & (row_devices - 1) == 0
    return (
        time_count == units == total == 4
        and power
        and rows % 512 == 0
        and block % 128 == 0
        and band % 256 == 0
    )


def local(event_counts, latent_mean, latent_var, eigen_basis, spectrum, correlation, whitened):
    time_count = lax.axis_size("tm")
    row_devices = lax.axis_size("row")
    here = lax.axis_index("tm")
    total = whitened.shape[3]
    block_modes = whitened.shape[2]
    band_width = eigen_basis.shape[1]
    if fits(event_counts, eigen_basis, whitened, time_count, row_devices):
        return fused(event_counts, latent_mean, latent_var, eigen_basis, spectrum, correlation, whitened)
    basis = lax.all_gather(eigen_basis, "row", axis=0, tiled=True)
    rows = event_counts.shape[1]
    row_chunks = ROW_CHUNKS if rows // ROW_CHUNKS % 128 == 0 else 1
    q_chunks = Q_CHUNKS if block_modes // Q_CHUNKS % 16 == 0 else 1
    step = rows // row_chunks
    parts = []
    for c in range(row_chunks):
        cut = [x[0, c * step : (c + 1) * step] for x in (event_counts, latent_mean, latent_var)]
        blocks = exchange_near(exchange_far(moments(*cut).astype(jnp.bfloat16), "tm"), "tm")
        parts.append([b for _, b in blocks])
    offsets = jnp.array([off for off, _ in blocks], jnp.int32)
    units = jnp.bitwise_xor(here.astype(jnp.int32), offsets)
    weights = jnp.take(time_factor(correlation[0], total), units, axis=0)
    halves = first_transform(parts, weights, basis, block_modes, q_chunks)
    scale_x = jnp.sqrt(lax.dynamic_slice_in_dim(spectrum, here * band_width, band_width, 0))[None, :]
    scale_y = jnp.sqrt(
        lax.dynamic_slice_in_dim(
            spectrum.reshape(time_count, row_devices, block_modes), lax.axis_index("row"), 1, 1
        ).reshape(time_count, block_modes, 1)
    )
    spread = []
    for h, half in enumerate(halves):
        if h >= 2:
            half = after(half, spread[h - 2][-1][1][0, 0, 0, 0])
        landed = lax.all_to_all(half, "row", split_axis=0, concat_axis=0, tiled=True)
        spread.append(exchange_far(landed, "tm"))
    gradient, done = None, None
    for h, blocks in enumerate(spread):
        if h == q_chunks - 1 and done is not None:
            blocks = blocks[:-1] + [(blocks[-1][0], after(blocks[-1][1], done[0, 0]))]
        groups = [b for _, b in exchange_near(blocks, "tm")]
        gradient, done = second_transform(
            groups, units, basis, scale_y, scale_x, whitened, gradient, h, q_chunks
        )
    return gradient


def solution(mesh):
    return jax.shard_map(
        local,
        mesh=mesh,
        in_specs=(
            P("tm", "row", None),
            P("tm", "row", None),
            P("tm", "row", None),
            P("row", "tm"),
            P(),
            P(),
            P(None, "row", None, None, "tm"),
        ),
        out_specs=P(None, "row", None, None, "tm"),
        check_vma=False,
    )
```

```python
import math

import jax
import jax.numpy as jnp
from jax import lax
from jax.experimental import pallas as pl
from jax.experimental.pallas import tpu as pltpu
from jax.sharding import PartitionSpec as P

HERMITE_NODES = (
    -2.0201828704560856,
    -0.9585724646138185,
    0.0,
    0.9585724646138185,
    2.0201828704560856,
)
HERMITE_WEIGHTS = (
    0.019953242059045913,
    0.3936193231522412,
    0.9453087204829419,
    0.3936193231522412,
    0.019953242059045913,
)


def moments(event_counts, latent_mean, latent_var):
    spread = jnp.sqrt(2.0 * latent_var)
    normal = 1.0 / math.sqrt(math.pi)
    points = [latent_mean + spread * abscissa for abscissa in HERMITE_NODES]
    rate_points = [jnp.exp(value) for value in points]
    mean_rate = sum(
        (weight * normal * value for weight, value in zip(HERMITE_WEIGHTS, rate_points))
    )
    covariance = sum(
        (
            weight * normal * (node_value - latent_mean) * (value - mean_rate)
            for weight, node_value, value in zip(HERMITE_WEIGHTS, points, rate_points)
        )
    )
    rate_var = sum(
        (
            weight * normal * (value - mean_rate) * (value - mean_rate)
            for weight, value in zip(HERMITE_WEIGHTS, rate_points)
        )
    )
    slope_gain = covariance / latent_var
    noise_var = rate_var - slope_gain * covariance + mean_rate
    return slope_gain * (event_counts.astype(latent_mean.dtype) - mean_rate) / noise_var


def time_factor(correlation, total):
    later = jnp.arange(total)[:, None]
    earlier = jnp.arange(total)[None, :]
    distance = jnp.maximum(later - earlier, 0).astype(correlation.dtype)
    lower = jnp.where(later >= earlier, jnp.power(correlation, distance), jnp.zeros_like(distance))
    column_scale = jnp.where(
        earlier == 0,
        jnp.ones_like(distance),
        jnp.sqrt(1.0 - correlation * correlation) * jnp.ones_like(distance),
    )
    return lower * column_scale


VMEM_BYTES = 60 * 1024 * 1024
ROW_CHUNKS = 2
Q_CHUNKS = 4


def after(block, value):
    return block + (value * 0.0).astype(block.dtype)


def exchange_step(blocks, axis, bit):
    pairs = [(i, i ^ bit) for i in range(lax.axis_size(axis))]
    return blocks + [(off ^ bit, lax.ppermute(b, axis, pairs)) for off, b in blocks]


def exchange_far(own, axis):
    half = lax.axis_size(axis) // 2
    return exchange_step([(0, own)], axis, half) if half else [(0, own)]


def exchange_near(blocks, axis):
    bit = lax.axis_size(axis) // 4
    while bit:
        blocks = exchange_step(blocks, axis, bit)
        bit //= 2
    return blocks


def first_transform(parts, weights, basis, block_modes, q_chunks):
    row_chunks, total = len(parts), len(parts[0])
    rows, width = parts[0][0].shape
    modes = basis.shape[1]
    tile = min(max(256, block_modes), modes)
    blocks = tile // block_modes
    sub = block_modes // q_chunks

    def kernel(weights_ref, *refs):
        part_refs = refs[: row_chunks * total]
        basis_ref = refs[row_chunks * total]
        out_refs = refs[row_chunks * total + 1 :]
        for c in range(row_chunks):
            fields = [
                jnp.dot(part_refs[c * total + t][...], basis_ref[...], preferred_element_type=jnp.float32)
                for t in range(total)
            ]
            for a in range(total):
                mixed = sum(weights_ref[t, a] * fields[t] for t in range(total))
                turned = mixed.T.astype(jnp.bfloat16).reshape(blocks, block_modes, rows)
                for h in range(q_chunks):
                    out_refs[h][:, a, :, pl.ds(c * rows, rows)] = turned[:, h * sub : (h + 1) * sub, :]

    flat = [p for chunk in parts for p in chunk]
    out = jax.ShapeDtypeStruct((modes // block_modes, total, sub, row_chunks * rows), jnp.bfloat16)
    return pl.pallas_call(
        kernel,
        grid=(modes // tile,),
        in_specs=[pl.BlockSpec(memory_space=pltpu.SMEM)]
        + [pl.BlockSpec((rows, width), lambda i: (0, 0), pipeline_mode=pl.Buffered(1)) for _ in flat]
        + [pl.BlockSpec((width, tile), lambda i: (0, i))],
        out_specs=[pl.BlockSpec((blocks, total, sub, row_chunks * rows), lambda i: (i, 0, 0, 0))] * q_chunks,
        out_shape=[out] * q_chunks,
        compiler_params=pltpu.CompilerParams(vmem_limit_bytes=VMEM_BYTES),
        cost_estimate=pl.CostEstimate(
            flops=2 * total * row_chunks * rows * width * modes,
            bytes_accessed=2 * (total * row_chunks * rows * (width + modes) + width * modes),
            transcendentals=0,
        ),
        name="first_transform",
    )(weights, *flat, basis)


def second_transform(groups, units, basis, scale_y, scale_x, whitened, previous, h, q_chunks):
    count = len(groups)
    sources, total, sub, depth = groups[0].shape
    units_total, _, block_modes, _, band = whitened.shape
    tile = min(256, band)
    width = basis.shape[0]

    def kernel(units_ref, *refs):
        group_refs = refs[:count]
        basis_ref, y_ref, x_ref, whitened_ref = refs[count : count + 4]
        out_ref, done_ref = refs[-2:]
        done_ref[...] = jnp.zeros_like(done_ref)
        for s in range(count):
            left = jnp.concatenate(
                [group_refs[s][r].reshape(total * sub, depth) for r in range(sources)], axis=1
            )
            values = jnp.dot(left, basis_ref[...], preferred_element_type=jnp.float32)
            u = units_ref[s]
            scale = y_ref[u] * x_ref[...]
            for a in range(total):
                out_ref[u, 0, :, a, :] = scale * values[a * sub : (a + 1) * sub] - whitened_ref[u, 0, :, a, :]

    field = pl.BlockSpec((units_total, 1, sub, total, tile), lambda i: (0, 0, h, 0, i))
    operands = [units, *groups, basis, scale_y, scale_x, whitened]
    in_specs = (
        [pl.BlockSpec(memory_space=pltpu.SMEM)]
        + [pl.BlockSpec(g.shape, lambda i: (0, 0, 0, 0), pipeline_mode=pl.Buffered(1)) for g in groups]
        + [
            pl.BlockSpec((width, tile), lambda i: (0, i)),
            pl.BlockSpec((units_total, sub, 1), lambda i: (0, h, 0)),
            pl.BlockSpec((1, tile), lambda i: (0, i)),
            field,
        ]
    )
    aliases = {}
    if previous is not None:
        aliases = {len(operands): 0}
        operands.append(previous)
        in_specs.append(pl.BlockSpec(memory_space=pl.ANY))
    return pl.pallas_call(
        kernel,
        grid=(band // tile,),
        in_specs=in_specs,
        out_specs=[field, pl.BlockSpec((8, 128), lambda i: (0, 0))],
        out_shape=[
            jax.ShapeDtypeStruct(whitened.shape, jnp.float32),
            jax.ShapeDtypeStruct((8, 128), jnp.float32),
        ],
        input_output_aliases=aliases,
        compiler_params=pltpu.CompilerParams(vmem_limit_bytes=VMEM_BYTES),
        cost_estimate=pl.CostEstimate(
            flops=2 * count * total * sub * width * band,
            bytes_accessed=2 * width * (band + count * total * sub) + 8 * count * total * sub * band,
            transcendentals=0,
        ),
        name="second_transform",
    )(*operands)


MESH = pl.DeviceIdType.MESH
FUSED_VMEM_BYTES = 67043328
MOMENT_ROWS = 32


def flip(value, mask, span):
    result, bit = 0, 1
    while bit < span:
        digit = lax.rem(lax.div(value, bit), 2)
        other = lax.rem(lax.div(mask, bit), 2) if not isinstance(mask, int) else mask // bit % 2
        result = result + lax.rem(digit + other, 2) * bit
        bit *= 2
    return result


def pseudo_block(counts, mean, var):
    spread = jnp.sqrt(2.0 * var)
    normal = 1.0 / math.sqrt(math.pi)
    h0 = HERMITE_WEIGHTS[2] * normal
    h1 = HERMITE_WEIGHTS[3] * normal
    h2 = HERMITE_WEIGHTS[4] * normal
    d1 = spread * HERMITE_NODES[3]
    d2 = spread * HERMITE_NODES[4]
    level = jnp.exp(mean)
    up1, down1 = jnp.exp(d1), jnp.exp(-d1)
    up2, down2 = jnp.exp(d2), jnp.exp(-d2)
    rate = h0 + h1 * (up1 + down1) + h2 * (up2 + down2)
    cov = (h1 * d1) * (up1 - down1) + (h2 * d2) * (up2 - down2)
    e0 = 1.0 - rate
    e1, e2, e3, e4 = up1 - rate, down1 - rate, up2 - rate, down2 - rate
    scatter = h0 * (e0 * e0) + h1 * (e1 * e1 + e2 * e2) + h2 * (e3 * e3 + e4 * e4)
    slope = cov / var
    noise = level * (scatter - slope * cov) + rate
    return slope * (counts.astype(jnp.float32) - level * rate) / noise


def fused_kernel(
    correlation,
    counts,
    mean,
    var,
    basis,
    spectrum_y,
    spectrum_x,
    whitened,
    out,
    pbuf,
    ebuf,
    hbuf,
    gbuf,
    acc,
    c_in,
    m_in,
    v_in,
    scale_y,
    in_sem,
    own_sem,
    acc_sem,
    self_sem,
    out_sem,
    px_s,
    px_r,
    pc_s,
    pc_r,
    pf_s,
    pf_r,
    eu_s,
    eu_r,
    ed_s,
    ed_r,
    ey_s,
    ey_r,
    ez_s,
    ez_r,
    at_s,
    at_r,
    gx_s,
    gx_r,
    gc_s,
    gc_r,
    gf_s,
    gf_r,
):
    total, rows, cells = pbuf.shape
    lines = hbuf.shape[0]
    band = 2 * ebuf.shape[2]
    block = scale_y.shape[1]
    span = hbuf.shape[-1]
    units = gbuf.shape[0]
    chunk = c_in.shape[1]
    chunks = rows // chunk
    half = rows // 2
    i = lax.axis_index("tm")
    r = lax.axis_index("row")
    z = lax.div(r, 2)
    y = lax.rem(r, 2)
    near = flip(i, 1, units)
    far = flip(i, 2, units)
    cross = flip(i, 3, units)
    side = 2 * z + 1 - y
    twin = flip(z, 1, lines)

    def remote(src, dst, send, recv, tm, row):
        return pltpu.make_async_remote_copy(
            src_ref=src, dst_ref=dst, send_sem=send, recv_sem=recv, device_id=(tm, row), device_id_type=MESH
        )

    def fetch(c):
        slot = lax.rem(c, 2)
        at = pl.ds(pl.multiple_of(c * chunk, chunk), chunk)
        return [
            pltpu.make_async_copy(src.at[0, at], dst.at[slot], in_sem.at[n, slot])
            for n, (src, dst) in enumerate(((counts, c_in), (mean, m_in), (var, v_in)))
        ]

    for c in range(2):
        for copy in fetch(c):
            copy.start()
    narrow = ebuf.shape[2]
    own_basis = [
        pltpu.make_async_copy(
            basis.at[:, pl.ds(ch * narrow, narrow)],
            ebuf.at[ch, pl.ds(pl.multiple_of(r * rows, rows), rows)],
            own_sem.at[ch],
        )
        for ch in range(2)
    ]
    for copy in own_basis:
        copy.start()
    fill = pltpu.make_async_copy(whitened.at[:, 0], acc, acc_sem)
    fill.start()

    barrier = pltpu.get_barrier_semaphore()
    for row in range(2 * lines - 1):
        peer = lax.rem(r + 1 + row, 2 * lines)
        pl.semaphore_signal(barrier, inc=1, device_id=(i, peer), device_id_type=MESH)
    for tm in (near, far):
        pl.semaphore_signal(barrier, inc=1, device_id=(tm, r), device_id_type=MESH)
    pl.semaphore_wait(barrier, 2 * lines + 1)

    above = lines - 1 - z
    hot = jnp.where(z < lines // 2, 1, 0)

    def piece(line, column, ch):
        return ebuf.at[ch, pl.ds(pl.multiple_of((2 * line + column) * rows, rows), rows)]

    def basis_up(line, ch, n, slot):
        ref = piece(line, y, ch)
        return remote(ref, ref, eu_s.at[n], eu_r.at[slot], i, r + 2)

    def basis_down(line, ch, n, slot):
        ref = piece(line, y, ch)
        return remote(ref, ref, ed_s.at[n], ed_r.at[slot], i, r - 2)

    def basis_side(line, column, ch):
        ref = piece(line, column, ch)
        return remote(ref, ref, ey_s.at[2 * line + ch], ey_r.at[2 * line + ch], i, side)

    def basis_cross(line, column):
        ref = piece(line, column, 1 - hot)
        return remote(ref, ref, ez_s, ez_r, i, 2 * twin + y)

    def own_up(second):
        return basis_up(z, second, second * (z + 1), second * (z + 1))

    def own_down(second):
        return basis_down(z, 1 - second, second * (above + 1), second * (above + 1))

    def below_step(m, action):
        @pl.when(m < 2 * z)
        def _():
            second = jnp.where(m >= z, 1, 0)
            b = m - second * z
            action(z - 1 - b, second, second * (z + 1) + b + 1)

    def above_step(m, action):
        @pl.when(m < 2 * above)
        def _():
            second = jnp.where(m >= above, 1, 0)
            b = m - second * above
            action(z + 1 + b, 1 - second, second * (above + 1) + b + 1)

    def relay(m):
        def from_below(line, ch, slot):
            basis_up(line, ch, slot, m).wait_recv()

            @pl.when(z < lines - 1)
            def _():
                basis_up(line, ch, slot, slot).start()

        def from_above(line, ch, slot):
            basis_down(line, ch, slot, m).wait_recv()

            @pl.when(z > 0)
            def _():
                basis_down(line, ch, slot, slot).start()

        below_step(m, from_below)

        @pl.when(jnp.logical_and(m == z - 1, z < lines - 1))
        def _():
            own_up(1).start()

        above_step(m, from_above)

        @pl.when(jnp.logical_and(m == above - 1, z > 0))
        def _():
            own_down(1).start()

    def beside(m, warm, begin):
        def go(line, ch, slot):
            right = ch == hot if warm else jnp.logical_and(ch != hot, line != twin)

            @pl.when(right)
            def _():
                copy = basis_side(line, y, ch)
                (copy.start if begin else copy.wait_send)()

        below_step(m, go)
        above_step(m, go)

    for copy in own_basis:
        copy.wait()

    @pl.when(z < lines - 1)
    def _():
        own_up(0).start()

    @pl.when(z > 0)
    def _():
        own_down(0).start()

    @pl.when(z == 0)
    def _():
        own_up(1).start()

    @pl.when(above == 0)
    def _():
        own_down(1).start()

    basis_side(z, y, hot).start()

    def set_scales():
        for u in range(units):
            line = jnp.sqrt(spectrum_y[u, pl.ds(r, 1), :])
            scale_y[u] = jnp.broadcast_to(line, (128, block)).T

    def rows_of(t, c):
        return pbuf.at[t, pl.ds(pl.multiple_of(c * chunk, chunk), chunk)]

    def slice_far(t, c):
        return remote(rows_of(t, c), rows_of(t, c), px_s.at[c], px_r.at[c], far, r)

    def slice_near(t, c):
        return remote(rows_of(t, c), rows_of(t, c), pc_s.at[c], pc_r.at[c], near, r)

    def slice_on(t, c):
        return remote(rows_of(t, c), rows_of(t, c), pf_s.at[c], pf_r.at[c], near, r)

    lanes = 512 if cells % 512 == 0 else 128
    per_row = cells // lanes

    def moment_step(c, _):
        slot = lax.rem(c, 2)
        for copy in fetch(c):
            copy.wait()

        def part(n, _):
            top = pl.multiple_of(lax.div(n, per_row) * 16, 16)
            left = pl.multiple_of(lax.rem(n, per_row) * lanes, lanes)
            at = (slot, pl.ds(top, 16), pl.ds(left, lanes))
            value = pseudo_block(c_in[at], m_in[at], v_in[at])
            pbuf[i, pl.ds(pl.multiple_of(c * chunk + top, 16), 16), pl.ds(left, lanes)] = value.astype(pbuf.dtype)
            return 0

        lax.fori_loop(0, 2, part, 0)

        @pl.when(c > 0)
        def _():
            slice_far(i, c - 1).start()
            slice_near(i, c - 1).start()

        lax.fori_loop(2, (chunk // 16) * per_row, part, 0)

        @pl.when(c + 2 < chunks)
        def _():
            for copy in fetch(c + 2):
                copy.start()

        return 0

    def pass_on(c, _):
        slice_far(far, c).wait_recv()
        slice_on(far, c).start()
        return 0

    def arrive(c, _):
        slice_near(near, c).wait_recv()
        slice_on(cross, c).wait_recv()
        return 0

    def transform(h, k):
        line = flip(z, k, lines)
        ch = lax.div(line, lines // 2)
        cols = pl.ds(pl.multiple_of(lax.rem(line, lines // 2) * (2 * block), 2 * block), 2 * block)
        at = pl.ds(pl.multiple_of(h * span, span), span)
        fields = [jnp.dot(pbuf[t, at, :], ebuf[ch, :, cols], preferred_element_type=jnp.float32) for t in range(total)]
        decay = correlation[0]
        gain = jnp.sqrt(jnp.full((1, 2 * block), 1.0 - decay * decay, jnp.float32))
        mixed = None
        for a in reversed(range(total)):
            mixed = fields[a] if mixed is None else fields[a] + decay * mixed
            turned = (gain * mixed if a else mixed).T.astype(hbuf.dtype)
            for column in range(2):
                hbuf[k, column, h, a * block : (a + 1) * block, :] = turned[column * block : (column + 1) * block]

    def column_of(other):
        return 1 - y if other else y

    def source(code):
        return 2 * flip(z, code // 2, lines) + column_of(code % 2)

    def push(h, k, other):
        code = 2 * k + other
        peer = 2 * flip(z, k, lines) + column_of(other)
        src = hbuf.at[k, column_of(other), h]
        return remote(src, gbuf.at[i, h, r], at_s.at[h, code], at_r.at[h, code], i, peer)

    def landed(h, code):
        src = hbuf.at[code // 2, column_of(code % 2), h]
        return remote(src, gbuf.at[i, h, source(code)], at_s.at[h, code], at_r.at[h, code], i, source(code))

    def block_far(u, h, code):
        ref = gbuf.at[u, h, source(code)]
        return remote(ref, ref, gx_s.at[h, code], gx_r.at[h, code], far, r)

    def block_near(u, h, code):
        ref = gbuf.at[u, h, source(code)]
        return remote(ref, ref, gc_s.at[h, code], gc_r.at[h, code], near, r)

    def block_on(u, h, code):
        ref = gbuf.at[u, h, source(code)]
        return remote(ref, ref, gf_s.at[h, code], gf_r.at[h, code], near, r)

    def spread(h, code):
        if code:
            landed(h, code).wait_recv()
        block_far(i, h, code).start()
        block_near(i, h, code).start()

    def cleanup(later):
        @pl.when(z < lines - 1)
        def _():
            own_up(0).wait_send()
            own_up(1).wait_send()

        @pl.when(z > 0)
        def _():
            own_down(0).wait_send()
            own_down(1).wait_send()

        basis_side(z, y, hot).wait_send()
        basis_side(z, y, 1 - hot).wait_send()
        for m in range(relays):

            def up_done(line, ch, slot):
                @pl.when(z < lines - 1)
                def _():
                    basis_up(line, ch, slot, slot).wait_send()

            def down_done(line, ch, slot):
                @pl.when(z > 0)
                def _():
                    basis_down(line, ch, slot, slot).wait_send()

            below_step(m, up_done)
            above_step(m, down_done)
            beside(m, True, False)
            beside(m, False, False)

        def sent(c, _):
            slice_far(i, c).wait_send()
            slice_near(i, c).wait_send()
            slice_on(far, c).wait_send()
            return 0

        basis_cross(z, 1 - y).wait_send()

        lax.fori_loop(0, chunks, sent, 0)
        if later:
            for h, code in sequence:
                if code:
                    push(h, code // 2, code % 2).wait_send()
                block_far(i, h, code).wait_send()
                block_near(i, h, code).wait_send()
                block_on(far, h, code).wait_send()

    wide = ebuf.shape[2]

    def accumulate(u, pair, first):
        def part(n, _):
            cols = pl.ds(pl.multiple_of(n * wide, wide), wide)
            values = None
            for h, code in pair:
                s = source(code)
                depth = pl.ds(pl.multiple_of(s * rows + h * span, span), span)
                term = jnp.dot(gbuf[u, h, s], ebuf[n, depth, :], preferred_element_type=jnp.float32)
                values = term if values is None else values + term
            left = pl.multiple_of(i * band + n * wide, wide)
            scale = scale_y[u, :, 0:1] * jnp.sqrt(spectrum_x[:, pl.ds(left, wide)])
            for a in range(total):
                term = scale * values[a * block : (a + 1) * block]
                if first:
                    acc[u, :, a, cols] = term - acc[u, :, a, cols]
                else:
                    acc[u, :, a, cols] = term + acc[u, :, a, cols]
            return 0

        lax.fori_loop(0, band // wide, part, 0)

    def tile(h, k):
        transform(h, k)
        push(h, k, 0).start()
        push(h, k, 1).start()

    def home(h):
        transform(h, 0)
        own = pltpu.make_async_copy(hbuf.at[0, y, h], gbuf.at[i, h, r], self_sem)
        own.start()
        push(h, 0, 1).start()
        own.wait()
        spread(h, 0)

    def tiles(h, first, last):
        def step(k, _):
            tile(h, k)
            return 0

        lax.fori_loop(first, last, step, 0)

    relays = 2 * (lines - 1)
    half_chunks = span // chunk
    mid = lines // 2
    warm = [2 * k + o for k in range(mid, lines) for o in (0, 1)]
    cool = [2 * k + o for k in range(mid) for o in (0, 1)]
    sequence = [(0, c) for c in warm] + [(0, 0), (0, 1), (1, 0)] + [(0, c) for c in cool[2:]]
    sequence += [(1, c) for c in warm[:2] + cool[1:] + warm[2:]]
    count = len(sequence)

    lax.fori_loop(0, chunks // 2, moment_step, 0)
    relay(0)
    beside(0, True, True)
    lax.fori_loop(chunks // 2, chunks, moment_step, 0)
    slice_far(i, chunks - 1).start()
    slice_near(i, chunks - 1).start()
    set_scales()
    done = 0
    for m in range(1, relays):
        if m == relays - 2:
            lax.fori_loop(done, half_chunks, pass_on, 0)
            done = half_chunks
            for line in range(lines):
                basis_side(line, 1 - y, hot).wait_recv()
            lax.fori_loop(0, half_chunks, arrive, 0)
            tiles(0, mid, lines)
        elif m == relays - 1:
            upto = min(chunks, max(done, 2 * m))
            lax.fori_loop(done, upto, pass_on, 0)
            done = upto
        relay(m)
        beside(m, True, True)
        if m == lines - 2:
            basis_side(z, y, 1 - hot).start()
            for before in range(m + 1):
                beside(before, False, True)
        elif m > lines - 2:
            beside(m, False, True)
        if m < relays - 2:
            upto = min(half_chunks, 2 * m + 1)
            lax.fori_loop(done, upto, pass_on, 0)
            done = upto
        if m == relays - 2:
            basis_side(z, 1 - y, 1 - hot).wait_recv()
            basis_cross(z, 1 - y).start()
    lax.fori_loop(done, chunks - 3, pass_on, 0)
    spread(*sequence[0])
    lax.fori_loop(chunks - 3, chunks - 2, pass_on, 0)
    spread(*sequence[1])
    lax.fori_loop(chunks - 2, chunks, pass_on, 0)
    lax.fori_loop(half_chunks, chunks, arrive, 0)
    tiles(1, mid, lines)
    spread(*sequence[2])
    spread(*sequence[3])
    for line in range(lines):

        @pl.when(jnp.logical_and(line != twin, line != z))
        def _():
            basis_side(line, 1 - y, 1 - hot).wait_recv()

    basis_cross(twin, 1 - y).wait_recv()

    def close(h, _):
        home(h)
        tiles(h, 1, mid)
        return 0

    lax.fori_loop(0, 2, close, 0)
    begun = 4
    fill.wait()

    def finish(u, n):
        return pltpu.make_async_copy(acc.at[u], out.at[u, 0], out_sem.at[n])

    pairs = [sequence[2 * p : 2 * p + 2] for p in range(count // 2)]
    groups = pairs[:-1] + [sequence[-2:-1], sequence[-1:]]
    state = {"passed": 0, "local": 0, "remote": 0}

    def forward(upto):
        while state["passed"] < upto:
            h, code = sequence[state["passed"]]
            block_far(far, h, code).wait_recv()
            block_on(far, h, code).start()
            state["passed"] += 1

    def local_pair():
        p = state["local"]
        for h, code in pairs[p]:
            block_near(near, h, code).wait_recv()
        for u in (i, near):
            accumulate(u, pairs[p], p == 0)
        state["local"] += 1

    def remote_pair():
        p = state["remote"]
        accumulate(far, groups[p], p == 0)
        for h, code in groups[p]:
            block_on(cross, h, code).wait_recv()
        accumulate(cross, groups[p], p == 0)
        state["remote"] += 1

    for n in range(begun, count):
        if sequence[n][1]:
            spread(*sequence[n])
        forward(max(0, n - 2))
        if 2 * state["local"] + 1 <= n:
            local_pair()
        if 2 * state["remote"] + 1 <= n - 3:
            remote_pair()
    while state["local"] < count // 2:
        local_pair()
    finish(i, 0).start()
    finish(near, 1).start()
    while state["remote"] < len(groups):
        forward(sum(len(g) for g in groups[: state["remote"] + 1]))
        remote_pair()
    finish(far, 2).start()
    finish(cross, 3).start()
    for n, u in enumerate((i, near, far, cross)):
        finish(u, n).wait()
    cleanup(True)


def fused(event_counts, latent_mean, latent_var, basis, spectrum, correlation, whitened):
    rows, cells = event_counts.shape[1:]
    units, _, block, total, band = whitened.shape
    sources = cells // rows
    lines = sources // 2
    chunks = rows // MOMENT_ROWS
    span = rows // 2
    dma = pltpu.SemaphoreType.DMA
    any_space = pl.BlockSpec(memory_space=pl.ANY)
    vmem = pl.BlockSpec(memory_space=pltpu.VMEM)
    result = pl.pallas_call(
        fused_kernel,
        in_specs=[pl.BlockSpec(memory_space=pltpu.SMEM)] + [any_space] * 4 + [vmem] * 2 + [any_space],
        out_specs=any_space,
        out_shape=jax.ShapeDtypeStruct(whitened.shape, jnp.float32),
        scratch_shapes=[
            pltpu.VMEM((total, rows, cells), jnp.bfloat16),
            pltpu.VMEM((2, cells, band // 2), jnp.bfloat16),
            pltpu.VMEM((lines, 2, 2, total * block, span), jnp.bfloat16),
            pltpu.VMEM((units, 2, sources, total * block, span), jnp.bfloat16),
            pltpu.VMEM((units, block, total, band), jnp.float32),
            pltpu.VMEM((2, MOMENT_ROWS, cells), jnp.int32),
            pltpu.VMEM((2, MOMENT_ROWS, cells), jnp.float32),
            pltpu.VMEM((2, MOMENT_ROWS, cells), jnp.float32),
            pltpu.VMEM((units, block, 128), jnp.float32),
            dma((3, 2)),
            dma((2,)),
            dma,
            dma,
            dma((4,)),
        ]
        + [dma((chunks,))] * 6
        + [dma((2 * lines,))] * 6
        + [dma] * 2
        + [dma((2, sources))] * 8,
        compiler_params=pltpu.CompilerParams(
            collective_id=0, has_side_effects=True, vmem_limit_bytes=FUSED_VMEM_BYTES
        ),
        cost_estimate=pl.CostEstimate(
            flops=4 * total * rows * cells * band,
            bytes_accessed=12 * rows * cells + 2 * rows * band + 8 * units * block * total * band,
            transcendentals=7 * rows * cells,
        ),
        name="cox_gradient",
    )(
        correlation,
        event_counts,
        latent_mean,
        latent_var,
        basis,
        spectrum.reshape(units, sources, block),
        spectrum[None, :],
        whitened,
    )
    return settle(result)


def settle(result):
    units, _, block, total, band = result.shape
    cuts = 2
    step = block // cuts

    def kernel(src, dst, held, in_sem, out_sem):
        def into(n):
            at = pl.ds(n % cuts * step, step)
            return pltpu.make_async_copy(src.at[n // cuts, 0, at], held.at[n], in_sem.at[n])

        def back(n):
            at = pl.ds(n % cuts * step, step)
            return pltpu.make_async_copy(held.at[n], dst.at[n // cuts, 0, at], out_sem.at[n])

        for n in range(units * cuts):
            into(n).start()
        for n in range(units * cuts):
            into(n).wait()
            back(n).start()
        for n in range(units * cuts):
            back(n).wait()

    return pl.pallas_call(
        kernel,
        in_specs=[pl.BlockSpec(memory_space=pl.ANY)],
        out_specs=pl.BlockSpec(memory_space=pl.ANY),
        out_shape=jax.ShapeDtypeStruct(result.shape, result.dtype),
        scratch_shapes=[
            pltpu.VMEM((units * cuts, step, total, band), result.dtype),
            pltpu.SemaphoreType.DMA((units * cuts,)),
            pltpu.SemaphoreType.DMA((units * cuts,)),
        ],
        compiler_params=pltpu.CompilerParams(vmem_limit_bytes=VMEM_BYTES),
        name="settle",
    )(result)


def fits(event_counts, eigen_basis, whitened, time_count, row_devices):
    rows = event_counts.shape[1]
    units, _, block, total, band = whitened.shape
    power = row_devices >= 4 and row_devices & (row_devices - 1) == 0
    return (
        time_count == units == total == 4
        and power
        and rows % 512 == 0
        and block % 128 == 0
        and band % 256 == 0
    )


def local(event_counts, latent_mean, latent_var, eigen_basis, spectrum, correlation, whitened):
    time_count = lax.axis_size("tm")
    row_devices = lax.axis_size("row")
    here = lax.axis_index("tm")
    total = whitened.shape[3]
    block_modes = whitened.shape[2]
    band_width = eigen_basis.shape[1]
    if fits(event_counts, eigen_basis, whitened, time_count, row_devices):
        return fused(event_counts, latent_mean, latent_var, eigen_basis, spectrum, correlation, whitened)
    basis = lax.all_gather(eigen_basis, "row", axis=0, tiled=True)
    rows = event_counts.shape[1]
    row_chunks = ROW_CHUNKS if rows // ROW_CHUNKS % 128 == 0 else 1
    q_chunks = Q_CHUNKS if block_modes // Q_CHUNKS % 16 == 0 else 1
    step = rows // row_chunks
    parts = []
    for c in range(row_chunks):
        cut = [x[0, c * step : (c + 1) * step] for x in (event_counts, latent_mean, latent_var)]
        blocks = exchange_near(exchange_far(moments(*cut).astype(jnp.bfloat16), "tm"), "tm")
        parts.append([b for _, b in blocks])
    offsets = jnp.array([off for off, _ in blocks], jnp.int32)
    units = jnp.bitwise_xor(here.astype(jnp.int32), offsets)
    weights = jnp.take(time_factor(correlation[0], total), units, axis=0)
    halves = first_transform(parts, weights, basis, block_modes, q_chunks)
    scale_x = jnp.sqrt(lax.dynamic_slice_in_dim(spectrum, here * band_width, band_width, 0))[None, :]
    scale_y = jnp.sqrt(
        lax.dynamic_slice_in_dim(
            spectrum.reshape(time_count, row_devices, block_modes), lax.axis_index("row"), 1, 1
        ).reshape(time_count, block_modes, 1)
    )
    spread = []
    for h, half in enumerate(halves):
        if h >= 2:
            half = after(half, spread[h - 2][-1][1][0, 0, 0, 0])
        landed = lax.all_to_all(half, "row", split_axis=0, concat_axis=0, tiled=True)
        spread.append(exchange_far(landed, "tm"))
    gradient, done = None, None
    for h, blocks in enumerate(spread):
        if h == q_chunks - 1 and done is not None:
            blocks = blocks[:-1] + [(blocks[-1][0], after(blocks[-1][1], done[0, 0]))]
        groups = [b for _, b in exchange_near(blocks, "tm")]
        gradient, done = second_transform(
            groups, units, basis, scale_y, scale_x, whitened, gradient, h, q_chunks
        )
    return gradient


def solution(mesh):
    return jax.shard_map(
        local,
        mesh=mesh,
        in_specs=(
            P("tm", "row", None),
            P("tm", "row", None),
            P("tm", "row", None),
            P("row", "tm"),
            P(),
            P(),
            P(None, "row", None, None, "tm"),
        ),
        out_specs=P(None, "row", None, None, "tm"),
        check_vma=False,
    )
```

```python
import math

import jax
import jax.numpy as jnp
from jax import lax
from jax.experimental import pallas as pl
from jax.experimental.pallas import tpu as pltpu
from jax.sharding import PartitionSpec as P

HERMITE_NODES = (
    -2.0201828704560856,
    -0.9585724646138185,
    0.0,
    0.9585724646138185,
    2.0201828704560856,
)
HERMITE_WEIGHTS = (
    0.019953242059045913,
    0.3936193231522412,
    0.9453087204829419,
    0.3936193231522412,
    0.019953242059045913,
)


def moments(event_counts, latent_mean, latent_var):
    spread = jnp.sqrt(2.0 * latent_var)
    normal = 1.0 / math.sqrt(math.pi)
    points = [latent_mean + spread * abscissa for abscissa in HERMITE_NODES]
    rate_points = [jnp.exp(value) for value in points]
    mean_rate = sum(
        (weight * normal * value for weight, value in zip(HERMITE_WEIGHTS, rate_points))
    )
    covariance = sum(
        (
            weight * normal * (node_value - latent_mean) * (value - mean_rate)
            for weight, node_value, value in zip(HERMITE_WEIGHTS, points, rate_points)
        )
    )
    rate_var = sum(
        (
            weight * normal * (value - mean_rate) * (value - mean_rate)
            for weight, value in zip(HERMITE_WEIGHTS, rate_points)
        )
    )
    slope_gain = covariance / latent_var
    noise_var = rate_var - slope_gain * covariance + mean_rate
    return slope_gain * (event_counts.astype(latent_mean.dtype) - mean_rate) / noise_var


def time_factor(correlation, total):
    later = jnp.arange(total)[:, None]
    earlier = jnp.arange(total)[None, :]
    distance = jnp.maximum(later - earlier, 0).astype(correlation.dtype)
    lower = jnp.where(later >= earlier, jnp.power(correlation, distance), jnp.zeros_like(distance))
    column_scale = jnp.where(
        earlier == 0,
        jnp.ones_like(distance),
        jnp.sqrt(1.0 - correlation * correlation) * jnp.ones_like(distance),
    )
    return lower * column_scale


VMEM_BYTES = 60 * 1024 * 1024
ROW_CHUNKS = 2
Q_CHUNKS = 4


def after(block, value):
    return block + (value * 0.0).astype(block.dtype)


def exchange_step(blocks, axis, bit):
    pairs = [(i, i ^ bit) for i in range(lax.axis_size(axis))]
    return blocks + [(off ^ bit, lax.ppermute(b, axis, pairs)) for off, b in blocks]


def exchange_far(own, axis):
    half = lax.axis_size(axis) // 2
    return exchange_step([(0, own)], axis, half) if half else [(0, own)]


def exchange_near(blocks, axis):
    bit = lax.axis_size(axis) // 4
    while bit:
        blocks = exchange_step(blocks, axis, bit)
        bit //= 2
    return blocks


def first_transform(parts, weights, basis, block_modes, q_chunks):
    row_chunks, total = len(parts), len(parts[0])
    rows, width = parts[0][0].shape
    modes = basis.shape[1]
    tile = min(max(256, block_modes), modes)
    blocks = tile // block_modes
    sub = block_modes // q_chunks

    def kernel(weights_ref, *refs):
        part_refs = refs[: row_chunks * total]
        basis_ref = refs[row_chunks * total]
        out_refs = refs[row_chunks * total + 1 :]
        for c in range(row_chunks):
            fields = [
                jnp.dot(part_refs[c * total + t][...], basis_ref[...], preferred_element_type=jnp.float32)
                for t in range(total)
            ]
            for a in range(total):
                mixed = sum(weights_ref[t, a] * fields[t] for t in range(total))
                turned = mixed.T.astype(jnp.bfloat16).reshape(blocks, block_modes, rows)
                for h in range(q_chunks):
                    out_refs[h][:, a, :, pl.ds(c * rows, rows)] = turned[:, h * sub : (h + 1) * sub, :]

    flat = [p for chunk in parts for p in chunk]
    out = jax.ShapeDtypeStruct((modes // block_modes, total, sub, row_chunks * rows), jnp.bfloat16)
    return pl.pallas_call(
        kernel,
        grid=(modes // tile,),
        in_specs=[pl.BlockSpec(memory_space=pltpu.SMEM)]
        + [pl.BlockSpec((rows, width), lambda i: (0, 0), pipeline_mode=pl.Buffered(1)) for _ in flat]
        + [pl.BlockSpec((width, tile), lambda i: (0, i))],
        out_specs=[pl.BlockSpec((blocks, total, sub, row_chunks * rows), lambda i: (i, 0, 0, 0))] * q_chunks,
        out_shape=[out] * q_chunks,
        compiler_params=pltpu.CompilerParams(vmem_limit_bytes=VMEM_BYTES),
        cost_estimate=pl.CostEstimate(
            flops=2 * total * row_chunks * rows * width * modes,
            bytes_accessed=2 * (total * row_chunks * rows * (width + modes) + width * modes),
            transcendentals=0,
        ),
        name="first_transform",
    )(weights, *flat, basis)


def second_transform(groups, units, basis, scale_y, scale_x, whitened, previous, h, q_chunks):
    count = len(groups)
    sources, total, sub, depth = groups[0].shape
    units_total, _, block_modes, _, band = whitened.shape
    tile = min(256, band)
    width = basis.shape[0]

    def kernel(units_ref, *refs):
        group_refs = refs[:count]
        basis_ref, y_ref, x_ref, whitened_ref = refs[count : count + 4]
        out_ref, done_ref = refs[-2:]
        done_ref[...] = jnp.zeros_like(done_ref)
        for s in range(count):
            left = jnp.concatenate(
                [group_refs[s][r].reshape(total * sub, depth) for r in range(sources)], axis=1
            )
            values = jnp.dot(left, basis_ref[...], preferred_element_type=jnp.float32)
            u = units_ref[s]
            scale = y_ref[u] * x_ref[...]
            for a in range(total):
                out_ref[u, 0, :, a, :] = scale * values[a * sub : (a + 1) * sub] - whitened_ref[u, 0, :, a, :]

    field = pl.BlockSpec((units_total, 1, sub, total, tile), lambda i: (0, 0, h, 0, i))
    operands = [units, *groups, basis, scale_y, scale_x, whitened]
    in_specs = (
        [pl.BlockSpec(memory_space=pltpu.SMEM)]
        + [pl.BlockSpec(g.shape, lambda i: (0, 0, 0, 0), pipeline_mode=pl.Buffered(1)) for g in groups]
        + [
            pl.BlockSpec((width, tile), lambda i: (0, i)),
            pl.BlockSpec((units_total, sub, 1), lambda i: (0, h, 0)),
            pl.BlockSpec((1, tile), lambda i: (0, i)),
            field,
        ]
    )
    aliases = {}
    if previous is not None:
        aliases = {len(operands): 0}
        operands.append(previous)
        in_specs.append(pl.BlockSpec(memory_space=pl.ANY))
    return pl.pallas_call(
        kernel,
        grid=(band // tile,),
        in_specs=in_specs,
        out_specs=[field, pl.BlockSpec((8, 128), lambda i: (0, 0))],
        out_shape=[
            jax.ShapeDtypeStruct(whitened.shape, jnp.float32),
            jax.ShapeDtypeStruct((8, 128), jnp.float32),
        ],
        input_output_aliases=aliases,
        compiler_params=pltpu.CompilerParams(vmem_limit_bytes=VMEM_BYTES),
        cost_estimate=pl.CostEstimate(
            flops=2 * count * total * sub * width * band,
            bytes_accessed=2 * width * (band + count * total * sub) + 8 * count * total * sub * band,
            transcendentals=0,
        ),
        name="second_transform",
    )(*operands)


MESH = pl.DeviceIdType.MESH
FUSED_VMEM_BYTES = 67043328
MOMENT_ROWS = 32


def flip(value, mask, span):
    result, bit = 0, 1
    while bit < span:
        digit = lax.rem(lax.div(value, bit), 2)
        other = lax.rem(lax.div(mask, bit), 2) if not isinstance(mask, int) else mask // bit % 2
        result = result + lax.rem(digit + other, 2) * bit
        bit *= 2
    return result


def pseudo_block(counts, mean, var):
    spread = jnp.sqrt(2.0 * var)
    normal = 1.0 / math.sqrt(math.pi)
    h0 = HERMITE_WEIGHTS[2] * normal
    h1 = HERMITE_WEIGHTS[3] * normal
    h2 = HERMITE_WEIGHTS[4] * normal
    d1 = spread * HERMITE_NODES[3]
    d2 = spread * HERMITE_NODES[4]
    level = jnp.exp(mean)
    up1, down1 = jnp.exp(d1), jnp.exp(-d1)
    up2, down2 = jnp.exp(d2), jnp.exp(-d2)
    rate = h0 + h1 * (up1 + down1) + h2 * (up2 + down2)
    cov = (h1 * d1) * (up1 - down1) + (h2 * d2) * (up2 - down2)
    e0 = 1.0 - rate
    e1, e2, e3, e4 = up1 - rate, down1 - rate, up2 - rate, down2 - rate
    scatter = h0 * (e0 * e0) + h1 * (e1 * e1 + e2 * e2) + h2 * (e3 * e3 + e4 * e4)
    slope = cov / var
    noise = level * (scatter - slope * cov) + rate
    return slope * (counts.astype(jnp.float32) - level * rate) / noise


def fused_kernel(
    correlation,
    counts,
    mean,
    var,
    basis,
    spectrum_y,
    spectrum_x,
    whitened,
    out,
    pbuf,
    ebuf,
    hbuf,
    gbuf,
    acc,
    c_in,
    m_in,
    v_in,
    scale_y,
    in_sem,
    own_sem,
    acc_sem,
    self_sem,
    out_sem,
    px_s,
    px_r,
    pc_s,
    pc_r,
    pf_s,
    pf_r,
    eu_s,
    eu_r,
    ed_s,
    ed_r,
    ey_s,
    ey_r,
    ez_s,
    ez_r,
    at_s,
    at_r,
    gx_s,
    gx_r,
    gc_s,
    gc_r,
    gf_s,
    gf_r,
):
    total, rows, cells = pbuf.shape
    lines = hbuf.shape[0]
    band = 2 * ebuf.shape[2]
    block = scale_y.shape[1]
    span = hbuf.shape[-1]
    units = gbuf.shape[0]
    chunk = c_in.shape[1]
    chunks = rows // chunk
    half = rows // 2
    i = lax.axis_index("tm")
    r = lax.axis_index("row")
    z = lax.div(r, 2)
    y = lax.rem(r, 2)
    near = flip(i, 1, units)
    far = flip(i, 2, units)
    cross = flip(i, 3, units)
    side = 2 * z + 1 - y
    twin = flip(z, 1, lines)

    def remote(src, dst, send, recv, tm, row):
        return pltpu.make_async_remote_copy(
            src_ref=src, dst_ref=dst, send_sem=send, recv_sem=recv, device_id=(tm, row), device_id_type=MESH
        )

    def fetch(c):
        slot = lax.rem(c, 2)
        at = pl.ds(pl.multiple_of(c * chunk, chunk), chunk)
        return [
            pltpu.make_async_copy(src.at[0, at], dst.at[slot], in_sem.at[n, slot])
            for n, (src, dst) in enumerate(((counts, c_in), (mean, m_in), (var, v_in)))
        ]

    for c in range(2):
        for copy in fetch(c):
            copy.start()
    narrow = ebuf.shape[2]
    own_basis = [
        pltpu.make_async_copy(
            basis.at[:, pl.ds(ch * narrow, narrow)],
            ebuf.at[ch, pl.ds(pl.multiple_of(r * rows, rows), rows)],
            own_sem.at[ch],
        )
        for ch in range(2)
    ]
    for copy in own_basis:
        copy.start()
    fill = pltpu.make_async_copy(whitened.at[:, 0], acc, acc_sem)
    fill.start()

    barrier = pltpu.get_barrier_semaphore()
    for row in range(2 * lines - 1):
        peer = lax.rem(r + 1 + row, 2 * lines)
        pl.semaphore_signal(barrier, inc=1, device_id=(i, peer), device_id_type=MESH)
    for tm in (near, far):
        pl.semaphore_signal(barrier, inc=1, device_id=(tm, r), device_id_type=MESH)
    pl.semaphore_wait(barrier, 2 * lines + 1)

    above = lines - 1 - z
    hot = jnp.where(z < lines // 2, 1, 0)

    def piece(line, column, ch):
        return ebuf.at[ch, pl.ds(pl.multiple_of((2 * line + column) * rows, rows), rows)]

    def basis_up(line, ch, n, slot):
        ref = piece(line, y, ch)
        return remote(ref, ref, eu_s.at[n], eu_r.at[slot], i, r + 2)

    def basis_down(line, ch, n, slot):
        ref = piece(line, y, ch)
        return remote(ref, ref, ed_s.at[n], ed_r.at[slot], i, r - 2)

    def basis_side(line, column, ch):
        ref = piece(line, column, ch)
        return remote(ref, ref, ey_s.at[2 * line + ch], ey_r.at[2 * line + ch], i, side)

    def basis_cross(line, column):
        ref = piece(line, column, 1 - hot)
        return remote(ref, ref, ez_s, ez_r, i, 2 * twin + y)

    def own_up(second):
        return basis_up(z, second, second * (z + 1), second * (z + 1))

    def own_down(second):
        return basis_down(z, 1 - second, second * (above + 1), second * (above + 1))

    def below_step(m, action):
        @pl.when(m < 2 * z)
        def _():
            second = jnp.where(m >= z, 1, 0)
            b = m - second * z
            action(z - 1 - b, second, second * (z + 1) + b + 1)

    def above_step(m, action):
        @pl.when(m < 2 * above)
        def _():
            second = jnp.where(m >= above, 1, 0)
            b = m - second * above
            action(z + 1 + b, 1 - second, second * (above + 1) + b + 1)

    def relay(m):
        def from_below(line, ch, slot):
            basis_up(line, ch, slot, m).wait_recv()

            @pl.when(z < lines - 1)
            def _():
                basis_up(line, ch, slot, slot).start()

        def from_above(line, ch, slot):
            basis_down(line, ch, slot, m).wait_recv()

            @pl.when(z > 0)
            def _():
                basis_down(line, ch, slot, slot).start()

        below_step(m, from_below)

        @pl.when(jnp.logical_and(m == z - 1, z < lines - 1))
        def _():
            own_up(1).start()

        above_step(m, from_above)

        @pl.when(jnp.logical_and(m == above - 1, z > 0))
        def _():
            own_down(1).start()

    def beside(m, warm, begin):
        def go(line, ch, slot):
            right = ch == hot if warm else jnp.logical_and(ch != hot, line != twin)

            @pl.when(right)
            def _():
                copy = basis_side(line, y, ch)
                (copy.start if begin else copy.wait_send)()

        below_step(m, go)
        above_step(m, go)

    for copy in own_basis:
        copy.wait()

    @pl.when(z < lines - 1)
    def _():
        own_up(0).start()

    @pl.when(z > 0)
    def _():
        own_down(0).start()

    @pl.when(z == 0)
    def _():
        own_up(1).start()

    @pl.when(above == 0)
    def _():
        own_down(1).start()

    basis_side(z, y, hot).start()

    def set_scales():
        for u in range(units):
            line = jnp.sqrt(spectrum_y[u, pl.ds(r, 1), :])
            scale_y[u] = jnp.broadcast_to(line, (128, block)).T

    def rows_of(t, c):
        return pbuf.at[t, pl.ds(pl.multiple_of(c * chunk, chunk), chunk)]

    def slice_far(t, c):
        return remote(rows_of(t, c), rows_of(t, c), px_s.at[c], px_r.at[c], far, r)

    def slice_near(t, c):
        return remote(rows_of(t, c), rows_of(t, c), pc_s.at[c], pc_r.at[c], near, r)

    def slice_on(t, c):
        return remote(rows_of(t, c), rows_of(t, c), pf_s.at[c], pf_r.at[c], near, r)

    lanes = 512 if cells % 512 == 0 else 128
    per_row = cells // lanes

    def moment_step(c, _):
        slot = lax.rem(c, 2)
        for copy in fetch(c):
            copy.wait()

        def part(n, _):
            top = pl.multiple_of(lax.div(n, per_row) * 16, 16)
            left = pl.multiple_of(lax.rem(n, per_row) * lanes, lanes)
            at = (slot, pl.ds(top, 16), pl.ds(left, lanes))
            value = pseudo_block(c_in[at], m_in[at], v_in[at])
            pbuf[i, pl.ds(pl.multiple_of(c * chunk + top, 16), 16), pl.ds(left, lanes)] = value.astype(pbuf.dtype)
            return 0

        lax.fori_loop(0, 2, part, 0)

        @pl.when(c > 0)
        def _():
            slice_far(i, c - 1).start()
            slice_near(i, c - 1).start()

        lax.fori_loop(2, (chunk // 16) * per_row, part, 0)

        @pl.when(c + 2 < chunks)
        def _():
            for copy in fetch(c + 2):
                copy.start()

        return 0

    def pass_on(c, _):
        slice_far(far, c).wait_recv()
        slice_on(far, c).start()
        return 0

    def arrive(c, _):
        slice_near(near, c).wait_recv()
        slice_on(cross, c).wait_recv()
        return 0

    def transform(h, k):
        line = flip(z, k, lines)
        ch = lax.div(line, lines // 2)
        cols = pl.ds(pl.multiple_of(lax.rem(line, lines // 2) * (2 * block), 2 * block), 2 * block)
        at = pl.ds(pl.multiple_of(h * span, span), span)
        fields = [jnp.dot(pbuf[t, at, :], ebuf[ch, :, cols], preferred_element_type=jnp.float32) for t in range(total)]
        decay = correlation[0]
        gain = jnp.sqrt(jnp.full((1, 2 * block), 1.0 - decay * decay, jnp.float32))
        mixed = None
        for a in reversed(range(total)):
            mixed = fields[a] if mixed is None else fields[a] + decay * mixed
            turned = (gain * mixed if a else mixed).T.astype(hbuf.dtype)
            for column in range(2):
                hbuf[k, column, h, a * block : (a + 1) * block, :] = turned[column * block : (column + 1) * block]

    def column_of(other):
        return 1 - y if other else y

    def source(code):
        return 2 * flip(z, code // 2, lines) + column_of(code % 2)

    def push(h, k, other):
        code = 2 * k + other
        peer = 2 * flip(z, k, lines) + column_of(other)
        src = hbuf.at[k, column_of(other), h]
        return remote(src, gbuf.at[i, h, r], at_s.at[h, code], at_r.at[h, code], i, peer)

    def landed(h, code):
        src = hbuf.at[code // 2, column_of(code % 2), h]
        return remote(src, gbuf.at[i, h, source(code)], at_s.at[h, code], at_r.at[h, code], i, source(code))

    def block_far(u, h, code):
        ref = gbuf.at[u, h, source(code)]
        return remote(ref, ref, gx_s.at[h, code], gx_r.at[h, code], far, r)

    def block_near(u, h, code):
        ref = gbuf.at[u, h, source(code)]
        return remote(ref, ref, gc_s.at[h, code], gc_r.at[h, code], near, r)

    def block_on(u, h, code):
        ref = gbuf.at[u, h, source(code)]
        return remote(ref, ref, gf_s.at[h, code], gf_r.at[h, code], near, r)

    def spread(h, code):
        if code:
            landed(h, code).wait_recv()
        block_far(i, h, code).start()
        block_near(i, h, code).start()

    def cleanup():
        @pl.when(z < lines - 1)
        def _():
            own_up(0).wait_send()
            own_up(1).wait_send()

        @pl.when(z > 0)
        def _():
            own_down(0).wait_send()
            own_down(1).wait_send()

        basis_side(z, y, hot).wait_send()
        basis_side(z, y, 1 - hot).wait_send()
        for m in range(relays):

            def up_done(line, ch, slot):
                @pl.when(z < lines - 1)
                def _():
                    basis_up(line, ch, slot, slot).wait_send()

            def down_done(line, ch, slot):
                @pl.when(z > 0)
                def _():
                    basis_down(line, ch, slot, slot).wait_send()

            below_step(m, up_done)
            above_step(m, down_done)
            beside(m, True, False)
            beside(m, False, False)

        def sent(c, _):
            slice_far(i, c).wait_send()
            slice_near(i, c).wait_send()
            slice_on(far, c).wait_send()
            return 0

        basis_cross(z, 1 - y).wait_send()

        lax.fori_loop(0, chunks, sent, 0)
        for h, code in sequence:
            if code:
                push(h, code // 2, code % 2).wait_send()

    def drain(part):
        for h, code in part:
            block_far(i, h, code).wait_send()
            block_near(i, h, code).wait_send()
            block_on(far, h, code).wait_send()

    wide = ebuf.shape[2]

    def accumulate(u, pair, first):
        def part(n, _):
            cols = pl.ds(pl.multiple_of(n * wide, wide), wide)
            values = None
            for h, code in pair:
                s = source(code)
                depth = pl.ds(pl.multiple_of(s * rows + h * span, span), span)
                term = jnp.dot(gbuf[u, h, s], ebuf[n, depth, :], preferred_element_type=jnp.float32)
                values = term if values is None else values + term
            left = pl.multiple_of(i * band + n * wide, wide)
            scale = scale_y[u, :, 0:1] * jnp.sqrt(spectrum_x[:, pl.ds(left, wide)])
            for a in range(total):
                term = scale * values[a * block : (a + 1) * block]
                if first:
                    acc[u, :, a, cols] = term - acc[u, :, a, cols]
                else:
                    acc[u, :, a, cols] = term + acc[u, :, a, cols]
            return 0

        lax.fori_loop(0, band // wide, part, 0)

    def tile(h, k):
        transform(h, k)
        push(h, k, 0).start()
        push(h, k, 1).start()

    def home(h):
        transform(h, 0)
        own = pltpu.make_async_copy(hbuf.at[0, y, h], gbuf.at[i, h, r], self_sem)
        own.start()
        push(h, 0, 1).start()
        own.wait()
        spread(h, 0)

    def tiles(h, first, last):
        def step(k, _):
            tile(h, k)
            return 0

        lax.fori_loop(first, last, step, 0)

    relays = 2 * (lines - 1)
    half_chunks = span // chunk
    mid = lines // 2
    warm = [2 * k + o for k in range(mid, lines) for o in (0, 1)]
    cool = [2 * k + o for k in range(mid) for o in (0, 1)]
    sequence = [(0, c) for c in warm] + [(0, 0), (0, 1), (1, 0)] + [(0, c) for c in cool[2:]]
    sequence += [(1, c) for c in warm[:2] + cool[1:] + warm[2:]]
    count = len(sequence)

    lax.fori_loop(0, 3 * chunks // 8, moment_step, 0)
    relay(0)
    beside(0, True, True)
    lax.fori_loop(3 * chunks // 8, 7 * chunks // 8, moment_step, 0)
    relay(1)
    beside(1, True, True)
    lax.fori_loop(7 * chunks // 8, chunks, moment_step, 0)
    slice_far(i, chunks - 1).start()
    slice_near(i, chunks - 1).start()
    set_scales()
    done = 0
    for m in range(1, relays):
        if m == relays - 2:
            lax.fori_loop(done, half_chunks, pass_on, 0)
            done = half_chunks
            for line in range(lines):
                basis_side(line, 1 - y, hot).wait_recv()
            lax.fori_loop(0, half_chunks, arrive, 0)
            tiles(0, mid, lines)
        elif m == relays - 1:
            upto = min(chunks, max(done, 2 * m))
            lax.fori_loop(done, upto, pass_on, 0)
            done = upto
        if m > 1:
            relay(m)
            beside(m, True, True)
        if m == lines - 2:
            basis_side(z, y, 1 - hot).start()
            for before in range(m + 1):
                beside(before, False, True)
        elif m > lines - 2:
            beside(m, False, True)
        if m < relays - 2:
            upto = min(half_chunks, 2 * m + 1)
            lax.fori_loop(done, upto, pass_on, 0)
            done = upto
        if m == relays - 2:
            basis_side(z, 1 - y, 1 - hot).wait_recv()
            basis_cross(z, 1 - y).start()
    lax.fori_loop(done, chunks - 3, pass_on, 0)
    spread(*sequence[0])
    lax.fori_loop(chunks - 3, chunks - 2, pass_on, 0)
    spread(*sequence[1])
    lax.fori_loop(chunks - 2, chunks, pass_on, 0)
    lax.fori_loop(half_chunks, chunks, arrive, 0)
    tiles(1, mid, lines)
    spread(*sequence[2])
    spread(*sequence[3])
    for line in range(lines):

        @pl.when(jnp.logical_and(line != twin, line != z))
        def _():
            basis_side(line, 1 - y, 1 - hot).wait_recv()

    basis_cross(twin, 1 - y).wait_recv()

    def close(h, _):
        home(h)
        tiles(h, 1, mid)
        return 0

    lax.fori_loop(0, 2, close, 0)
    begun = 4
    fill.wait()

    def finish(u, n):
        return pltpu.make_async_copy(acc.at[u], out.at[u, 0], out_sem.at[n])

    pairs = [sequence[2 * p : 2 * p + 2] for p in range(count // 2)]
    groups = pairs[:-1] + [sequence[-2:-1], sequence[-1:]]
    state = {"passed": 0, "local": 0, "remote": 0}

    def forward(upto):
        while state["passed"] < upto:
            h, code = sequence[state["passed"]]
            block_far(far, h, code).wait_recv()
            block_on(far, h, code).start()
            state["passed"] += 1

    def local_pair():
        p = state["local"]
        for h, code in pairs[p]:
            block_near(near, h, code).wait_recv()
        for u in (i, near):
            accumulate(u, pairs[p], p == 0)
        state["local"] += 1

    def remote_pair():
        p = state["remote"]
        accumulate(far, groups[p], p == 0)
        for h, code in groups[p]:
            block_on(cross, h, code).wait_recv()
        accumulate(cross, groups[p], p == 0)
        state["remote"] += 1

    for n in range(begun, count):
        if sequence[n][1]:
            spread(*sequence[n])
        forward(max(0, n - 2))
        if 2 * state["local"] + 1 <= n:
            local_pair()
        if 2 * state["remote"] + 1 <= n - 3:
            remote_pair()
    while state["local"] < count // 2:
        local_pair()
    finish(i, 0).start()
    finish(near, 1).start()
    cleanup()
    early = state["passed"]
    drain(sequence[:early])
    while state["remote"] < len(groups):
        forward(sum(len(g) for g in groups[: state["remote"] + 1]))
        remote_pair()
    finish(far, 2).start()
    finish(cross, 3).start()
    for n, u in enumerate((i, near, far, cross)):
        finish(u, n).wait()
    drain(sequence[early:])


def fused(event_counts, latent_mean, latent_var, basis, spectrum, correlation, whitened):
    rows, cells = event_counts.shape[1:]
    units, _, block, total, band = whitened.shape
    sources = cells // rows
    lines = sources // 2
    chunks = rows // MOMENT_ROWS
    span = rows // 2
    dma = pltpu.SemaphoreType.DMA
    any_space = pl.BlockSpec(memory_space=pl.ANY)
    vmem = pl.BlockSpec(memory_space=pltpu.VMEM)
    result = pl.pallas_call(
        fused_kernel,
        in_specs=[pl.BlockSpec(memory_space=pltpu.SMEM)] + [any_space] * 4 + [vmem] * 2 + [any_space],
        out_specs=any_space,
        out_shape=jax.ShapeDtypeStruct(whitened.shape, jnp.float32),
        scratch_shapes=[
            pltpu.VMEM((total, rows, cells), jnp.bfloat16),
            pltpu.VMEM((2, cells, band // 2), jnp.bfloat16),
            pltpu.VMEM((lines, 2, 2, total * block, span), jnp.bfloat16),
            pltpu.VMEM((units, 2, sources, total * block, span), jnp.bfloat16),
            pltpu.VMEM((units, block, total, band), jnp.float32),
            pltpu.VMEM((2, MOMENT_ROWS, cells), jnp.int32),
            pltpu.VMEM((2, MOMENT_ROWS, cells), jnp.float32),
            pltpu.VMEM((2, MOMENT_ROWS, cells), jnp.float32),
            pltpu.VMEM((units, block, 128), jnp.float32),
            dma((3, 2)),
            dma((2,)),
            dma,
            dma,
            dma((4,)),
        ]
        + [dma((chunks,))] * 6
        + [dma((2 * lines,))] * 6
        + [dma] * 2
        + [dma((2, sources))] * 8,
        compiler_params=pltpu.CompilerParams(
            collective_id=0, has_side_effects=True, vmem_limit_bytes=FUSED_VMEM_BYTES
        ),
        cost_estimate=pl.CostEstimate(
            flops=4 * total * rows * cells * band,
            bytes_accessed=12 * rows * cells + 2 * rows * band + 8 * units * block * total * band,
            transcendentals=7 * rows * cells,
        ),
        name="cox_gradient",
    )(
        correlation,
        event_counts,
        latent_mean,
        latent_var,
        basis,
        spectrum.reshape(units, sources, block),
        spectrum[None, :],
        whitened,
    )
    return settle(result)


def settle(result):
    units, _, block, total, band = result.shape
    cuts = 2
    step = block // cuts

    def kernel(src, dst, held, in_sem, out_sem):
        def into(n):
            at = pl.ds(n % cuts * step, step)
            return pltpu.make_async_copy(src.at[n // cuts, 0, at], held.at[n], in_sem.at[n])

        def back(n):
            at = pl.ds(n % cuts * step, step)
            return pltpu.make_async_copy(held.at[n], dst.at[n // cuts, 0, at], out_sem.at[n])

        for n in range(units * cuts):
            into(n).start()
        for n in range(units * cuts):
            into(n).wait()
            back(n).start()
        for n in range(units * cuts):
            back(n).wait()

    return pl.pallas_call(
        kernel,
        in_specs=[pl.BlockSpec(memory_space=pl.ANY)],
        out_specs=pl.BlockSpec(memory_space=pl.ANY),
        out_shape=jax.ShapeDtypeStruct(result.shape, result.dtype),
        scratch_shapes=[
            pltpu.VMEM((units * cuts, step, total, band), result.dtype),
            pltpu.SemaphoreType.DMA((units * cuts,)),
            pltpu.SemaphoreType.DMA((units * cuts,)),
        ],
        compiler_params=pltpu.CompilerParams(vmem_limit_bytes=VMEM_BYTES),
        name="settle",
    )(result)


def fits(event_counts, eigen_basis, whitened, time_count, row_devices):
    rows = event_counts.shape[1]
    units, _, block, total, band = whitened.shape
    power = row_devices >= 4 and row_devices & (row_devices - 1) == 0
    return (
        time_count == units == total == 4
        and power
        and rows % 512 == 0
        and block % 128 == 0
        and band % 256 == 0
    )


def local(event_counts, latent_mean, latent_var, eigen_basis, spectrum, correlation, whitened):
    time_count = lax.axis_size("tm")
    row_devices = lax.axis_size("row")
    here = lax.axis_index("tm")
    total = whitened.shape[3]
    block_modes = whitened.shape[2]
    band_width = eigen_basis.shape[1]
    if fits(event_counts, eigen_basis, whitened, time_count, row_devices):
        return fused(event_counts, latent_mean, latent_var, eigen_basis, spectrum, correlation, whitened)
    basis = lax.all_gather(eigen_basis, "row", axis=0, tiled=True)
    rows = event_counts.shape[1]
    row_chunks = ROW_CHUNKS if rows // ROW_CHUNKS % 128 == 0 else 1
    q_chunks = Q_CHUNKS if block_modes // Q_CHUNKS % 16 == 0 else 1
    step = rows // row_chunks
    parts = []
    for c in range(row_chunks):
        cut = [x[0, c * step : (c + 1) * step] for x in (event_counts, latent_mean, latent_var)]
        blocks = exchange_near(exchange_far(moments(*cut).astype(jnp.bfloat16), "tm"), "tm")
        parts.append([b for _, b in blocks])
    offsets = jnp.array([off for off, _ in blocks], jnp.int32)
    units = jnp.bitwise_xor(here.astype(jnp.int32), offsets)
    weights = jnp.take(time_factor(correlation[0], total), units, axis=0)
    halves = first_transform(parts, weights, basis, block_modes, q_chunks)
    scale_x = jnp.sqrt(lax.dynamic_slice_in_dim(spectrum, here * band_width, band_width, 0))[None, :]
    scale_y = jnp.sqrt(
        lax.dynamic_slice_in_dim(
            spectrum.reshape(time_count, row_devices, block_modes), lax.axis_index("row"), 1, 1
        ).reshape(time_count, block_modes, 1)
    )
    spread = []
    for h, half in enumerate(halves):
        if h >= 2:
            half = after(half, spread[h - 2][-1][1][0, 0, 0, 0])
        landed = lax.all_to_all(half, "row", split_axis=0, concat_axis=0, tiled=True)
        spread.append(exchange_far(landed, "tm"))
    gradient, done = None, None
    for h, blocks in enumerate(spread):
        if h == q_chunks - 1 and done is not None:
            blocks = blocks[:-1] + [(blocks[-1][0], after(blocks[-1][1], done[0, 0]))]
        groups = [b for _, b in exchange_near(blocks, "tm")]
        gradient, done = second_transform(
            groups, units, basis, scale_y, scale_x, whitened, gradient, h, q_chunks
        )
    return gradient


def solution(mesh):
    return jax.shard_map(
        local,
        mesh=mesh,
        in_specs=(
            P("tm", "row", None),
            P("tm", "row", None),
            P("tm", "row", None),
            P("row", "tm"),
            P(),
            P(),
            P(None, "row", None, None, "tm"),
        ),
        out_specs=P(None, "row", None, None, "tm"),
        check_vma=False,
    )
```
